8 devices in a mesh: dp: 2 (over z, y), sp: 4 (over x, core).
Axes of the slice: x: 2, y: 2, z: 1, core: 2. Of those that a mesh axis runs over, the one named last changes fastest.
Arguments:
- x: bfloat16 [32, 1024, 768], P('dp', 'sp'), parts along dimension 0
- g: bfloat16 [32, 1024, 768], P('dp', 'sp'), parts along dimension 0
- ln_g: float32 [768], replicated
- ln_b: float32 [768], replicated
- w_qkv: bfloat16 [768, 3, 12, 64], replicated
- b_qkv: float32 [3, 12, 64], replicated
- w_out: bfloat16 [12, 64, 768], replicated
- b_out: float32 [768], replicated
Outputs:
- output 1: bfloat16 [32, 1024, 768], P('dp', 'sp'), parts along dimension 0
- output 2: bfloat16 [32, 1024, 768], P('dp', 'sp'), parts along dimension 0
- output 3: float32 [1536], P('dp'), parts along dimension 0
- output 4: float32 [1536], P('dp'), parts along dimension 0
- output 5: float32 [1536, 3, 12, 64], P('dp'), parts along dimension 0
- output 6: float32 [6, 12, 64], P('dp'), parts along dimension 0
- output 7: float32 [24, 64, 768], P('dp'), parts along dimension 0
- output 8: float32 [1536], P('dp'), parts along dimension 0
There are 2 independent parts. The reference program is written for one: setup_inputs(seed, part) draws one part's arguments, and reference() takes and returns one part's arrays. A program takes and returns all parts, laid end to end along the dimension named above; an argument that names none is the same for every part.
All inputs are finite; a program needn't handle non-finite values.
Results may differ from the reference program's by a relative error of at most 0.00827913.
Values are sent between devices in bfloat16 or wider.
A program may use at most 1 GiB of HBM per device.

```python
import jax
import jax.numpy as jnp
from jax import lax

BATCH_SIZE = 16
SEQ_LEN = 1024
MODEL_DIM = 768
NUM_HEADS = 12
HEAD_DIM = 64
LN_EPS = 1e-5
QK_GAIN = 1.5
ROW_BLOCK = min(SEQ_LEN, 256)


def setup_inputs(seed: int = 0, part: int = 0) -> dict:
    shared = jax.random.split(jax.random.key(seed), 6)
    per_part = jax.random.split(jax.random.fold_in(jax.random.key(seed + 1), part), 2)
    tokens = (BATCH_SIZE, SEQ_LEN, MODEL_DIM)
    x = jax.random.normal(per_part[0], tokens, jnp.float32).astype(jnp.bfloat16)
    g = jax.random.normal(per_part[1], tokens, jnp.float32).astype(jnp.bfloat16)
    ln_g = 1.0 + 0.3 * jax.random.normal(shared[0], (MODEL_DIM,), jnp.float32)
    ln_b = 0.3 * jax.random.normal(shared[1], (MODEL_DIM,), jnp.float32)
    head_gain = jnp.array([QK_GAIN, QK_GAIN, 1.0], jnp.float32).reshape(1, 3, 1, 1)
    w_qkv = (jax.random.normal(shared[2], (MODEL_DIM, 3, NUM_HEADS, HEAD_DIM), jnp.float32) * head_gain * MODEL_DIM ** -0.5).astype(jnp.bfloat16)
    b_qkv = 0.3 * jax.random.normal(shared[3], (3, NUM_HEADS, HEAD_DIM), jnp.float32)
    w_out = (jax.random.normal(shared[4], (NUM_HEADS, HEAD_DIM, MODEL_DIM), jnp.float32) * MODEL_DIM ** -0.5).astype(jnp.bfloat16)
    b_out = 0.3 * jax.random.normal(shared[5], (MODEL_DIM,), jnp.float32)
    return {'x': x, 'g': g, 'ln_g': ln_g, 'ln_b': ln_b, 'w_qkv': w_qkv, 'b_qkv': b_qkv, 'w_out': w_out, 'b_out': b_out}


def layer_norm(x_in):
    x_f = x_in.astype(jnp.float32)
    centred = x_f - jnp.mean(x_f, axis=-1, keepdims=True)
    inv_std = lax.rsqrt(jnp.mean(centred * centred, axis=-1, keepdims=True) + LN_EPS)
    return centred * inv_std, inv_std


def block_probs(q_rows, keys, row_start):
    scores = jnp.einsum('bqhe,bkhe->bhqk', q_rows, keys) * HEAD_DIM ** -0.5
    row_pos = row_start + jnp.arange(q_rows.shape[1])
    col_pos = jnp.arange(keys.shape[1])
    scores = jnp.where(col_pos[None, :] <= row_pos[:, None], scores, -jnp.inf)
    return jax.nn.softmax(scores, axis=-1)


def attend_head(query, keys, values):
    def one_block(block_idx):
        row_start = block_idx * ROW_BLOCK
        q_rows = lax.dynamic_slice_in_dim(query, row_start, ROW_BLOCK, axis=1)
        attn_prob = block_probs(q_rows, keys, row_start).astype(jnp.bfloat16).astype(jnp.float32)
        return jnp.einsum('bhqk,bkhe->bqhe', attn_prob, values).astype(jnp.bfloat16)
    out_blocks = lax.map(one_block, jnp.arange(SEQ_LEN // ROW_BLOCK))
    return jnp.moveaxis(out_blocks, 0, 1).reshape(query.shape)


def attend_head_grad(query, keys, values, d_out):
    scale = HEAD_DIM ** -0.5
    def step(acc_pair, block_idx):
        key_grad, value_grad = acc_pair
        row_start = block_idx * ROW_BLOCK
        q_rows = lax.dynamic_slice_in_dim(query, row_start, ROW_BLOCK, axis=1)
        d_rows = lax.dynamic_slice_in_dim(d_out, row_start, ROW_BLOCK, axis=1)
        attn_prob = block_probs(q_rows, keys, row_start)
        d_prob = jnp.einsum('bqhe,bkhe->bhqk', d_rows, values)
        row_dot = jnp.sum(attn_prob * d_prob, axis=-1, keepdims=True)
        d_score = (attn_prob * (d_prob - row_dot) * scale).astype(jnp.bfloat16).astype(jnp.float32)
        prob_low = attn_prob.astype(jnp.bfloat16).astype(jnp.float32)
        q_grad = jnp.einsum('bhqk,bkhe->bqhe', d_score, keys).astype(jnp.bfloat16)
        key_grad = key_grad + jnp.einsum('bhqk,bqhe->bkhe', d_score, q_rows)
        value_grad = value_grad + jnp.einsum('bhqk,bqhe->bkhe', prob_low, d_rows)
        return (key_grad, value_grad), q_grad
    zeros = jnp.zeros(keys.shape, jnp.float32)
    (key_grad, value_grad), q_blocks = lax.scan(step, (zeros, zeros), jnp.arange(SEQ_LEN // ROW_BLOCK))
    q_grad = jnp.moveaxis(q_blocks, 0, 1).reshape(query.shape)
    return jnp.concatenate([q_grad, key_grad.astype(jnp.bfloat16), value_grad.astype(jnp.bfloat16)], axis=2)


def reference(x, g, ln_g, ln_b, w_qkv, b_qkv, w_out, b_out):
    x_hat, inv_std = layer_norm(x)
    hidden = (x_hat * ln_g + ln_b).astype(jnp.bfloat16).astype(jnp.float32)
    proj_qkv = (jnp.einsum('bsd,dthe->bsthe', hidden, w_qkv.astype(jnp.float32)) + b_qkv).astype(jnp.bfloat16)
    per_head = jnp.moveaxis(proj_qkv, 3, 0).astype(jnp.float32)

    def head_forward(head_in):
        return attend_head(head_in[:, :, 0:1], head_in[:, :, 1:2], head_in[:, :, 2:3])

    attn_out = jnp.moveaxis(lax.map(head_forward, per_head)[:, :, :, 0], 0, 2).astype(jnp.float32)
    out_proj = jnp.einsum('bshe,hed->bsd', attn_out, w_out.astype(jnp.float32)) + b_out
    y = (x.astype(jnp.float32) + out_proj).astype(jnp.bfloat16)

    g_f = g.astype(jnp.float32)
    d_b_out = jnp.sum(g_f, axis=(0, 1))
    d_w_out = jnp.einsum('bshe,bsd->hed', attn_out, g_f)
    d_attn = jnp.einsum('bsd,hed->bshe', g_f, w_out.astype(jnp.float32)).astype(jnp.bfloat16)
    d_per_head = jnp.moveaxis(d_attn, 2, 0)[:, :, :, None].astype(jnp.float32)

    def head_backward(pair):
        head_in, d_head = pair
        return attend_head_grad(head_in[:, :, 0:1], head_in[:, :, 1:2], head_in[:, :, 2:3], d_head)

    d_qkv = jnp.moveaxis(lax.map(head_backward, (per_head, d_per_head)), 0, 3).astype(jnp.float32)
    d_b_qkv = jnp.sum(d_qkv, axis=(0, 1))
    d_w_qkv = jnp.einsum('bsd,bsthe->dthe', hidden, d_qkv)
    d_hidden = jnp.einsum('bsthe,dthe->bsd', d_qkv, w_qkv.astype(jnp.float32))
    d_ln_g = jnp.sum(d_hidden * x_hat, axis=(0, 1))
    d_ln_b = jnp.sum(d_hidden, axis=(0, 1))
    d_norm = d_hidden * ln_g
    d_norm_in = inv_std * (d_norm - jnp.mean(d_norm, axis=-1, keepdims=True) - x_hat * jnp.mean(d_norm * x_hat, axis=-1, keepdims=True))
    d_x = (g_f + d_norm_in).astype(jnp.bfloat16)
    return (y, d_x, d_ln_g, d_ln_b, d_w_qkv, d_b_qkv, d_w_out, d_b_out)
```

```python
import functools

import jax
import jax.numpy as jnp
from jax import lax
from jax.experimental import pallas as pl
from jax.experimental.pallas import tpu as pltpu
from jax.sharding import PartitionSpec as P


LN_EPS = 1e-5
F32 = jnp.float32
BF16 = jnp.bfloat16
CHUNKS = 4
UP = [(0, 2), (1, 3)]
DOWN = [(2, 0), (3, 1)]
SWAP_CHIP = [(0, 2), (1, 3), (2, 0), (3, 1)]
SWAP_CORE = [(0, 1), (1, 0), (2, 3), (3, 2)]


UNREAD = pl.BlockSpec(memory_space=pltpu.HBM)


def dot_nn(a, b):
    return lax.dot_general(a, b, (((1,), (0,)), ((), ())), preferred_element_type=F32)


def dot_nt(a, b):
    return lax.dot_general(a, b, (((1,), (1,)), ((), ())), preferred_element_type=F32)


def params(n):
    return pltpu.CompilerParams(dimension_semantics=("arbitrary",) * n, vmem_limit_bytes=56 * 1024 * 1024)


def normed(x_f):
    centred = x_f - jnp.mean(x_f, axis=-1, keepdims=True)
    inv_std = lax.rsqrt(jnp.mean(centred * centred, axis=-1, keepdims=True) + LN_EPS)
    return centred * inv_std, inv_std


def front_kernel(core_ref, x_ref, xr_ref, g_ref, gr_ref, lng_ref, lnb_ref, w_ref, b_ref, wo_ref,
                 h_ref, q_ref, k_ref, v_ref, da_ref, xb_ref, gb_ref):
    dim = x_ref.shape[2]
    run = x_ref.shape[1]
    mine = pl.ds(pl.multiple_of(core_ref[0] * run, run), run)
    theirs = pl.ds(pl.multiple_of((1 - core_ref[0]) * run, run), run)
    xb_ref[0, mine, :] = x_ref[0]
    xb_ref[0, theirs, :] = xr_ref[0]
    gb_ref[0, mine, :] = g_ref[0]
    gb_ref[0, theirs, :] = gr_ref[0]
    da_ref[0] = dot_nt(gb_ref[0], wo_ref[...]).astype(BF16)
    x_hat, _ = normed(xb_ref[0].astype(F32))
    h_ref[0] = (x_hat * lng_ref[...] + lnb_ref[...]).astype(BF16)
    for t, out in enumerate((q_ref, k_ref, v_ref)):
        cols = slice(t * dim, (t + 1) * dim)
        out[0] = (dot_nt(h_ref[0], w_ref[cols, :]) + b_ref[:, cols]).astype(BF16)


def front(core, x, x_r, g, g_r, ln_g, ln_b, w_t, b_qkv, w_o, lo):
    batch, run, dim = x.shape
    n, seq = x_r.shape[0], 2 * run
    whole = lambda shape: pl.BlockSpec(shape, lambda b, c: (0,) * len(shape))
    own = pl.BlockSpec((1, run, dim), lambda b, c: (c[0] * (batch // 2) + lo + b, 0, 0))
    got = pl.BlockSpec((1, run, dim), lambda b, c: (b, 0, 0))
    tok = pl.BlockSpec((1, seq, dim), lambda b, c: (b, 0, 0))
    out = jax.ShapeDtypeStruct((n, seq, dim), BF16)
    return pl.pallas_call(
        front_kernel,
        grid_spec=pltpu.PrefetchScalarGridSpec(
            num_scalar_prefetch=1,
            grid=(n,),
            in_specs=[own, got, own, got, whole((1, dim)), whole((1, dim)), whole((3 * dim, dim)), whole((1, 3 * dim)), whole((dim, dim))],
            out_specs=[tok] * 7,
        ),
        out_shape=[out] * 7,
        compiler_params=params(1),
        cost_estimate=pl.CostEstimate(flops=8 * n * seq * dim * dim, bytes_accessed=18 * n * seq * dim, transcendentals=0),
        name="front",
    )(core, x, x_r, g, g_r, ln_g, ln_b, w_t, b_qkv, w_o)


def kv_kernel(role_ref, h_ref, w_ref, b_ref, k_ref, v_ref):
    dim = h_ref.shape[2]

    @pl.when(role_ref[0] == 1)
    def _():
        for t, out in enumerate((k_ref, v_ref)):
            cols = slice((t + 1) * dim, (t + 2) * dim)
            out[0] = (dot_nt(h_ref[0], w_ref[cols, :]) + b_ref[:, cols]).astype(BF16)


def other_kv(role, h_o, w_t, b_qkv):
    n, seq, dim = h_o.shape
    tok = pl.BlockSpec((1, seq, dim), lambda b, r: (b * r[0], 0, 0))
    out = jax.ShapeDtypeStruct((n, seq, dim), BF16)
    return pl.pallas_call(
        kv_kernel,
        grid_spec=pltpu.PrefetchScalarGridSpec(
            num_scalar_prefetch=1,
            grid=(n,),
            in_specs=[tok, pl.BlockSpec((3 * dim, dim), lambda b, r: (0, 0)), pl.BlockSpec((1, 3 * dim), lambda b, r: (0, 0))],
            out_specs=[tok] * 2,
        ),
        out_shape=[out] * 2,
        compiler_params=params(1),
        cost_estimate=pl.CostEstimate(flops=4 * n * seq * dim * dim, bytes_accessed=6 * n * seq * dim, transcendentals=0),
        name="other_kv",
    )(role, h_o, w_t, b_qkv)


def attn_kernel(role_ref, q_ref, k_ref, v_ref, g_ref, ko_ref, vo_ref, a_ref, dq_ref, dk_ref, dv_ref, st_ref, *, head, scale):
    seq = q_ref.shape[1]
    blk = seq // 2
    width = q_ref.shape[2]
    lane = lax.broadcasted_iota(jnp.int32, (blk, width), 1)
    causal = lax.broadcasted_iota(jnp.int32, (blk, blk), 0) <= lax.broadcasted_iota(jnp.int32, (blk, blk), 1)

    def run(rect):
        k_t, v_t = k_ref[0].T, v_ref[0].T
        if rect:
            ko_t, vo_t = ko_ref[0].T, vo_ref[0].T
        for qi in range(2):
            rows = slice(qi * blk, (qi + 1) * blk)
            q2 = q_ref[0, rows, :] * jnp.asarray(scale, BF16)
            g2 = g_ref[0, rows, :]
            o_parts, dq_parts = [], []
            dk_parts = [None] * (qi + 1)
            dv_parts = [None] * (qi + 1)
            for h in range(width // head):
                mine = (lane >= h * head) & (lane < (h + 1) * head)
                hrow = slice(h * head, (h + 1) * head)
                qm = jnp.where(mine, q2, jnp.zeros_like(q2))
                gm = jnp.where(mine, g2, jnp.zeros_like(g2))
                pieces = []
                for ki in range(qi + 1):
                    kr = slice(ki * blk, (ki + 1) * blk)
                    pieces.append((ki, k_ref[0, kr, :], v_ref[0, kr, :], k_t[hrow, kr], v_t[hrow, kr]))
                if rect:
                    for ki in range(2):
                        kr = slice(ki * blk, (ki + 1) * blk)
                        pieces.append((None, ko_ref[0, kr, :], vo_ref[0, kr, :], ko_t[hrow, kr], vo_t[hrow, kr]))
                s = []
                for ki, k_i, _, _, _ in pieces:
                    s_i = dot_nt(k_i, qm)
                    if ki == qi:
                        s_i = jnp.where(causal, s_i, -jnp.inf)
                    s.append(s_i)
                m = functools.reduce(jnp.maximum, [jnp.max(s_i, axis=0, keepdims=True) for s_i in s])
                e = [jnp.exp(s_i - m) for s_i in s]
                dp = [dot_nt(v_i, gm) for _, _, v_i, _, _ in pieces]
                l = functools.reduce(jnp.add, [jnp.sum(e_i, axis=0, keepdims=True) for e_i in e])
                c = functools.reduce(jnp.add, [jnp.sum(e_i * d_i, axis=0, keepdims=True) for e_i, d_i in zip(e, dp)])
                inv_l = 1.0 / l
                c = c * inv_l
                st_ref[0, 0, 2 * h, rows] = (m + jnp.log(l))[0]
                st_ref[0, 0, 2 * h + 1, rows] = c[0]
                o_h = dq_h = None
                for (ki, _, _, kt_i, vt_i), e_i, d_i in zip(pieces, e, dp):
                    p_i = e_i * inv_l
                    pb = p_i.astype(BF16)
                    ds = (p_i * (d_i - c)).astype(BF16)
                    o_i = dot_nn(vt_i, pb)
                    dq_i = dot_nn(kt_i, ds)
                    o_h = o_i if o_h is None else o_h + o_i
                    dq_h = dq_i if dq_h is None else dq_h + dq_i
                    if ki is not None:
                        dv_i = dot_nn(pb, gm)
                        dk_i = dot_nn(ds, qm)
                        dv_parts[ki] = dv_i if dv_parts[ki] is None else dv_parts[ki] + dv_i
                        dk_parts[ki] = dk_i if dk_parts[ki] is None else dk_parts[ki] + dk_i
                o_parts.append(o_h)
                dq_parts.append(dq_h)
            a_ref[0, rows, :] = jnp.concatenate(o_parts, axis=0).T.astype(BF16)
            dq_ref[0, rows, :] = (jnp.concatenate(dq_parts, axis=0).T * scale).astype(BF16)
            for ki in range(qi + 1):
                kr = slice(ki * blk, (ki + 1) * blk)
                if ki == qi:
                    dk_ref[0, kr, :] = dk_parts[ki]
                    dv_ref[0, kr, :] = dv_parts[ki]
                else:
                    dk_ref[0, kr, :] += dk_parts[ki]
                    dv_ref[0, kr, :] += dv_parts[ki]

    pl.when(role_ref[0] == 0)(lambda: run(False))
    pl.when(role_ref[0] == 1)(lambda: run(True))


def attend(role, q, k, v, da, k_o, v_o, head):
    n, seq, dim = q.shape
    width = 128
    pairs = dim // width
    tok = pl.BlockSpec((1, seq, width), lambda b, p, r: (b, 0, p))
    far = pl.BlockSpec((1, seq, width), lambda b, p, r: (b * r[0], 0, p * r[0]))
    low = jax.ShapeDtypeStruct((n, seq, dim), BF16)
    acc = jax.ShapeDtypeStruct((n, seq, dim), F32)
    return pl.pallas_call(
        functools.partial(attn_kernel, head=head, scale=head ** -0.5),
        grid_spec=pltpu.PrefetchScalarGridSpec(
            num_scalar_prefetch=1,
            grid=(n, pairs),
            in_specs=[tok] * 4 + [far] * 2,
            out_specs=[tok] * 4 + [pl.BlockSpec((1, 1, 4, seq), lambda b, p, r: (b, p, 0, 0))],
        ),
        out_shape=[low, low, acc, acc, jax.ShapeDtypeStruct((n, pairs, 4, seq), F32)],
        compiler_params=params(2),
        cost_estimate=pl.CostEstimate(flops=32 * n * seq * seq * dim, bytes_accessed=24 * n * seq * dim, transcendentals=0),
        name="attend",
    )(role, q, k, v, da, k_o, v_o)


def late_kernel(role_ref, q_ref, g_ref, st_ref, k_ref, v_ref, dka_ref, dva_ref, *rest, head, scale):
    dk_ref, dv_ref = rest[-2:]
    seq = q_ref.shape[1]
    blk = seq // 2
    width = q_ref.shape[2]
    lane = lax.broadcasted_iota(jnp.int32, (blk, width), 1)

    @pl.when(role_ref[0] == 1)
    def _():
        dk_ref[0] = dka_ref[0].astype(BF16)
        dv_ref[0] = dva_ref[0].astype(BF16)

    @pl.when(role_ref[0] == 0)
    def _():
        for ki in range(2):
            kr = slice(ki * blk, (ki + 1) * blk)
            k_i, v_i = k_ref[0, kr, :], v_ref[0, kr, :]
            dk, dv = dka_ref[0, kr, :], dva_ref[0, kr, :]
            for qi in range(2):
                rows = slice(qi * blk, (qi + 1) * blk)
                q2 = q_ref[0, rows, :] * jnp.asarray(scale, BF16)
                g2 = g_ref[0, rows, :]
                for h in range(width // head):
                    mine = (lane >= h * head) & (lane < (h + 1) * head)
                    qm = jnp.where(mine, q2, jnp.zeros_like(q2))
                    gm = jnp.where(mine, g2, jnp.zeros_like(g2))
                    lse = st_ref[0, 0, 2 * h, rows].reshape(1, blk)
                    c = st_ref[0, 0, 2 * h + 1, rows].reshape(1, blk)
                    p = jnp.exp(dot_nt(k_i, qm) - lse)
                    ds = (p * (dot_nt(v_i, gm) - c)).astype(BF16)
                    dv = dv + dot_nn(p.astype(BF16), gm)
                    dk = dk + dot_nn(ds, qm)
            dk_ref[0, kr, :] = dk.astype(BF16)
            dv_ref[0, kr, :] = dv.astype(BF16)


def late(role, q_o, da_o, stats, k, v, dk_acc, dv_acc, head, after):
    n, seq, dim = k.shape
    width = 128
    pairs = dim // width
    tok = pl.BlockSpec((1, seq, width), lambda b, p, r: (b, 0, p))
    far = pl.BlockSpec((1, seq, width), lambda b, p, r: (b * (1 - r[0]), 0, p * (1 - r[0])))
    low = jax.ShapeDtypeStruct((n, seq, dim), BF16)
    return pl.pallas_call(
        functools.partial(late_kernel, head=head, scale=head ** -0.5),
        grid_spec=pltpu.PrefetchScalarGridSpec(
            num_scalar_prefetch=1,
            grid=(n, pairs),
            in_specs=[far, far, pl.BlockSpec((1, 1, 4, seq), lambda b, p, r: (b, p, 0, 0)), far, far, tok, tok] + [UNREAD] * len(after),
            out_specs=[tok] * 2,
        ),
        out_shape=[low] * 2,
        compiler_params=params(2),
        cost_estimate=pl.CostEstimate(flops=16 * n * seq * seq * dim, bytes_accessed=20 * n * seq * dim, transcendentals=0),
        name="late",
    )(role, q_o, da_o, stats, k, v, dk_acc, dv_acc, *after)


def split_rows(core_ref, full_ref, own_ref, send_ref):
    run = own_ref.shape[1]
    own_ref[0] = full_ref[pl.ds(pl.multiple_of(core_ref[0] * run, run), run), :]
    send_ref[0] = full_ref[pl.ds(pl.multiple_of((1 - core_ref[0]) * run, run), run), :]


def post_kernel(core_ref, a_ref, x_ref, wo_ref, bo_ref, own_ref, send_ref, full_ref):
    out = dot_nn(a_ref[0], wo_ref[...]) + bo_ref[...]
    full_ref[...] = (x_ref[0].astype(F32) + out).astype(BF16)
    split_rows(core_ref, full_ref, own_ref, send_ref)


def post(core, a, x, w_o, b_o):
    n, seq, dim = a.shape
    run = seq // 2
    tok = pl.BlockSpec((1, seq, dim), lambda b, c: (b, 0, 0))
    part = pl.BlockSpec((1, run, dim), lambda b, c: (b, 0, 0))
    whole = lambda shape: pl.BlockSpec(shape, lambda b, c: (0,) * len(shape))
    return pl.pallas_call(
        post_kernel,
        grid_spec=pltpu.PrefetchScalarGridSpec(
            num_scalar_prefetch=1,
            grid=(n,),
            in_specs=[tok, tok, whole((dim, dim)), whole((1, dim))],
            out_specs=[part] * 2,
            scratch_shapes=[pltpu.VMEM((seq, dim), BF16)],
        ),
        out_shape=[jax.ShapeDtypeStruct((n, run, dim), BF16)] * 2,
        compiler_params=params(1),
        cost_estimate=pl.CostEstimate(flops=2 * n * seq * dim * dim, bytes_accessed=6 * n * seq * dim, transcendentals=0),
        name="post",
    )(core, a, x, w_o, b_o)


def back_kernel(core_ref, dq_ref, dk_ref, dv_ref, x_ref, g_ref, lng_ref, w_ref, prev_ref, *rest):
    own_ref, send_ref, acc_ref, full_ref = rest[-4:]
    dim = x_ref.shape[2]

    @pl.when(pl.program_id(0) == 0)
    def _():
        acc_ref[...] = prev_ref[...]

    dh = dot_nn(dq_ref[0], w_ref[0:dim, :]) + dot_nn(dk_ref[0], w_ref[dim:2 * dim, :]) + dot_nn(dv_ref[0], w_ref[2 * dim:3 * dim, :])
    x_hat, inv_std = normed(x_ref[0].astype(F32))
    g = g_ref[0].astype(F32)
    u = dh * lng_ref[...]
    dx = inv_std * (u - jnp.mean(u, axis=-1, keepdims=True) - x_hat * jnp.mean(u * x_hat, axis=-1, keepdims=True))
    full_ref[...] = (g + dx).astype(BF16)
    split_rows(core_ref, full_ref, own_ref, send_ref)
    acc_ref[0:1, :] += jnp.sum(dh * x_hat, axis=0, keepdims=True)
    acc_ref[1:2, :] += jnp.sum(dh, axis=0, keepdims=True)
    for t, ref in enumerate((dq_ref, dk_ref, dv_ref)):
        acc_ref[2 + t:3 + t, :] += jnp.sum(ref[0].astype(F32), axis=0, keepdims=True)
    acc_ref[5:6, :] += jnp.sum(g, axis=0, keepdims=True)


def back(core, dq, dk, dv, x, g, ln_g, w_t, prev, after):
    n, seq, dim = dq.shape
    run = seq // 2
    tok = pl.BlockSpec((1, seq, dim), lambda b, c: (b, 0, 0))
    part = pl.BlockSpec((1, run, dim), lambda b, c: (b, 0, 0))
    whole = lambda shape: pl.BlockSpec(shape, lambda b, c: (0,) * len(shape))
    return pl.pallas_call(
        back_kernel,
        grid_spec=pltpu.PrefetchScalarGridSpec(
            num_scalar_prefetch=1,
            grid=(n,),
            in_specs=[tok] * 5 + [whole((1, dim)), whole((3 * dim, dim)), whole((8, dim))] + [UNREAD] * len(after),
            out_specs=[part, part, whole((8, dim))],
            scratch_shapes=[pltpu.VMEM((seq, dim), BF16)],
        ),
        out_shape=[jax.ShapeDtypeStruct((n, run, dim), BF16)] * 2 + [jax.ShapeDtypeStruct((8, dim), F32)],
        compiler_params=params(1),
        cost_estimate=pl.CostEstimate(flops=6 * n * seq * dim * dim, bytes_accessed=12 * n * seq * dim, transcendentals=0),
        name="back",
    )(core, dq, dk, dv, x, g, ln_g, w_t, prev, *after)


def tok_dot(a, b):
    return lax.dot_general(a, b, (((0, 1), (0, 1)), ((), ())), preferred_element_type=F32)


def solution(mesh):
    tok_spec = P('dp', 'sp', None)
    part_spec = P('dp')

    def local_step(x, g, ln_g, ln_b, w_qkv, b_qkv, w_out, b_out):
        batch, run, dim = x.shape
        _, _, heads, head = w_qkv.shape
        index = lax.axis_index('sp')
        chip, core = lax.div(index, 2), lax.rem(index, 2)
        role, side = chip.reshape(1), core.reshape(1)
        ln_g2, ln_b2, b_o = ln_g.reshape(1, dim), ln_b.reshape(1, dim), b_out.reshape(1, dim)
        w_t = jnp.transpose(w_qkv, (1, 2, 3, 0)).reshape(3 * dim, dim)
        w_o = w_out.reshape(dim, dim)
        b_all = b_qkv.reshape(1, 3 * dim)
        half_b = batch // 2
        n = half_b // CHUNKS
        half_d = dim // 2

        def send(z, perm):
            return lax.ppermute(z, 'sp', perm)

        def handed(z, i):
            return send(lax.dynamic_slice_in_dim(z, (1 - core) * half_b + i * n, n, 0), SWAP_CORE)

        def gathered(own, got):
            buf = jnp.zeros((batch, run, dim), BF16)
            for i in range(CHUNKS):
                buf = lax.dynamic_update_slice_in_dim(buf, own[i], core * half_b + i * n, 0)
            for i in range(CHUNKS):
                buf = lax.dynamic_update_slice_in_dim(buf, got[i], (1 - core) * half_b + i * n, 0)
            return buf

        got = [(handed(g, i), handed(x, i)) for i in range(CHUNKS)]
        own, far = [], []
        for i in range(CHUNKS):
            h, q, k, v, da, xb, gb = front(side, x, got[i][1], g, got[i][0], ln_g2, ln_b2, w_t, b_all, w_o, i * n)
            own.append((h, q, k, v, da, xb, gb))
            far.append((send(h, UP), send(da, DOWN), send(q, DOWN)))

        att, y_own, y_send, dw_o, dw_q = [], [], [], None, None
        for i in range(CHUNKS):
            h, q, k, v, da, xb, gb = own[i]
            k_o, v_o = other_kv(role, far[i][0], w_t, b_all)
            a, dq, dk_acc, dv_acc, stats = attend(role, q, k, v, da, k_o, v_o, head)
            att.append((dq, dk_acc, dv_acc, send(stats, DOWN)))
            mine, theirs = post(side, a, xb, w_o, b_o)
            y_own.append(mine)
            y_send.append(theirs)
            do, dwq = tok_dot(a, gb), tok_dot(dq, h)
            dw_o = do if dw_o is None else dw_o + do
            dw_q = dwq if dw_q is None else dw_q + dwq

        def halves_added(w):
            theirs = send(lax.dynamic_slice_in_dim(w, (1 - core) * half_d, half_d, 0), SWAP_CORE)
            return lax.dynamic_slice_in_dim(w, core * half_d, half_d, 0) + theirs

        part_o, part_q = halves_added(dw_o), halves_added(dw_q)
        sum_o = part_o + send(part_o, SWAP_CHIP)
        sum_q = part_q + send(part_q, SWAP_CHIP)
        y = gathered(y_own, [send(z, SWAP_CORE) for z in y_send])

        dx_own, dx_send, dw_k, dw_v = [], [], None, None
        acc = jnp.zeros((8, dim), F32)
        after = [part_o, part_q] + y_send
        for i in range(CHUNKS):
            h, q, k, v, da, xb, gb = own[i]
            dq, dk_acc, dv_acc, stats_o = att[i]
            dk, dv = late(role, far[i][2], far[i][1], stats_o, k, v, dk_acc, dv_acc, head, after)
            dwk, dwv = tok_dot(dk, h), tok_dot(dv, h)
            dw_k = dwk if dw_k is None else dw_k + dwk
            dw_v = dwv if dw_v is None else dw_v + dwv
            if i == CHUNKS - 1:
                part_k, part_v = halves_added(dw_k), halves_added(dw_v)
                after = [part_k, part_v]
            else:
                after = [dwk, dwv]
            mine, theirs, acc = back(side, dq, dk, dv, xb, gb, ln_g2, w_t, acc, after)
            after = [acc]
            dx_own.append(mine)
            dx_send.append(theirs)
        sum_k = part_k + send(part_k, SWAP_CHIP)
        sum_v = part_v + send(part_v, SWAP_CHIP)
        d_x = gathered(dx_own, [send(z, SWAP_CORE) for z in dx_send])
        acc = acc + send(acc, SWAP_CORE)
        acc = acc + send(acc, SWAP_CHIP)

        d_w_out = jnp.zeros((dim, dim), F32)
        d_w_out = lax.dynamic_update_slice(d_w_out, sum_o, (core * half_d, 0))
        d_w_out = lax.dynamic_update_slice(d_w_out, send(sum_o, SWAP_CORE), ((1 - core) * half_d, 0))
        dw = jnp.zeros((3 * dim, dim), F32)
        for t, w in enumerate((sum_q, sum_k, sum_v)):
            dw = lax.dynamic_update_slice(dw, w, (t * dim + core * half_d, 0))
            dw = lax.dynamic_update_slice(dw, send(w, SWAP_CORE), (t * dim + (1 - core) * half_d, 0))
        d_w_qkv = jnp.transpose(dw.reshape(3, heads, head, dim), (3, 0, 1, 2))
        return y, d_x, acc[0], acc[1], d_w_qkv, acc[2:5].reshape(3, heads, head), d_w_out.reshape(heads, head, dim), acc[5]


    return jax.shard_map(local_step, mesh=mesh, in_specs=(tok_spec, tok_spec) + (P(),) * 6, out_specs=(tok_spec, tok_spec) + (part_spec,) * 6, check_vma=False)
```

```python
import functools

import jax
import jax.numpy as jnp
from jax import lax
from jax.experimental import pallas as pl
from jax.experimental.pallas import tpu as pltpu
from jax.sharding import PartitionSpec as P


LN_EPS = 1e-5
F32 = jnp.float32
BF16 = jnp.bfloat16
CHUNKS = 4
UP = [(0, 2), (1, 3)]
DOWN = [(2, 0), (3, 1)]
SWAP_CHIP = [(0, 2), (1, 3), (2, 0), (3, 1)]
SWAP_CORE = [(0, 1), (1, 0), (2, 3), (3, 2)]


UNREAD = pl.BlockSpec(memory_space=pltpu.HBM)


def dot_nn(a, b):
    return lax.dot_general(a, b, (((1,), (0,)), ((), ())), preferred_element_type=F32)


def dot_nt(a, b):
    return lax.dot_general(a, b, (((1,), (1,)), ((), ())), preferred_element_type=F32)


def params(n):
    return pltpu.CompilerParams(dimension_semantics=("arbitrary",) * n, vmem_limit_bytes=56 * 1024 * 1024)


def normed(x_f):
    centred = x_f - jnp.mean(x_f, axis=-1, keepdims=True)
    inv_std = lax.rsqrt(jnp.mean(centred * centred, axis=-1, keepdims=True) + LN_EPS)
    return centred * inv_std, inv_std


def front_kernel(core_ref, x_ref, xr_ref, g_ref, gr_ref, lng_ref, lnb_ref, w_ref, b_ref, wo_ref,
                 h_ref, qd_ref, k_ref, v_ref, xb_ref, gb_ref):
    dim = x_ref.shape[2]
    run = x_ref.shape[1]
    mine = pl.ds(pl.multiple_of(core_ref[0] * run, run), run)
    theirs = pl.ds(pl.multiple_of((1 - core_ref[0]) * run, run), run)
    xb_ref[0, mine, :] = x_ref[0]
    xb_ref[0, theirs, :] = xr_ref[0]
    gb_ref[0, mine, :] = g_ref[0]
    gb_ref[0, theirs, :] = gr_ref[0]
    qd_ref[0, 0] = dot_nt(gb_ref[0], wo_ref[...]).astype(BF16)
    x_hat, _ = normed(xb_ref[0].astype(F32))
    h_ref[0] = (x_hat * lng_ref[...] + lnb_ref[...]).astype(BF16)
    for t in range(3):
        cols = slice(t * dim, (t + 1) * dim)
        val = (dot_nt(h_ref[0], w_ref[cols, :]) + b_ref[:, cols]).astype(BF16)
        if t == 0:
            qd_ref[1, 0] = val
        else:
            (k_ref if t == 1 else v_ref)[0] = val


def front(core, x, x_r, g, g_r, ln_g, ln_b, w_t, b_qkv, w_o, lo):
    batch, run, dim = x.shape
    n, seq = x_r.shape[0], 2 * run
    whole = lambda shape: pl.BlockSpec(shape, lambda b, c: (0,) * len(shape))
    own = pl.BlockSpec((1, run, dim), lambda b, c: (c[0] * (batch // 2) + lo + b, 0, 0))
    got = pl.BlockSpec((1, run, dim), lambda b, c: (b, 0, 0))
    tok = pl.BlockSpec((1, seq, dim), lambda b, c: (b, 0, 0))
    out = jax.ShapeDtypeStruct((n, seq, dim), BF16)
    return pl.pallas_call(
        front_kernel,
        grid_spec=pltpu.PrefetchScalarGridSpec(
            num_scalar_prefetch=1,
            grid=(n,),
            in_specs=[own, got, own, got, whole((1, dim)), whole((1, dim)), whole((3 * dim, dim)), whole((1, 3 * dim)), whole((dim, dim))],
            out_specs=[tok, pl.BlockSpec((2, 1, seq, dim), lambda b, c: (0, b, 0, 0)), tok, tok, tok, tok],
        ),
        out_shape=[out, jax.ShapeDtypeStruct((2, n, seq, dim), BF16), out, out, out, out],
        compiler_params=params(1),
        cost_estimate=pl.CostEstimate(flops=8 * n * seq * dim * dim, bytes_accessed=18 * n * seq * dim, transcendentals=0),
        name="front",
    )(core, x, x_r, g, g_r, ln_g, ln_b, w_t, b_qkv, w_o)


def kv_kernel(role_ref, h_ref, w_ref, b_ref, k_ref, v_ref):
    dim = h_ref.shape[2]

    @pl.when(role_ref[0] == 1)
    def _():
        for t, out in enumerate((k_ref, v_ref)):
            cols = slice((t + 1) * dim, (t + 2) * dim)
            out[0] = (dot_nt(h_ref[0], w_ref[cols, :]) + b_ref[:, cols]).astype(BF16)


def other_kv(role, h_o, w_t, b_qkv):
    n, seq, dim = h_o.shape
    tok = pl.BlockSpec((1, seq, dim), lambda b, r: (b * r[0], 0, 0))
    out = jax.ShapeDtypeStruct((n, seq, dim), BF16)
    return pl.pallas_call(
        kv_kernel,
        grid_spec=pltpu.PrefetchScalarGridSpec(
            num_scalar_prefetch=1,
            grid=(n,),
            in_specs=[tok, pl.BlockSpec((3 * dim, dim), lambda b, r: (0, 0)), pl.BlockSpec((1, 3 * dim), lambda b, r: (0, 0))],
            out_specs=[tok] * 2,
        ),
        out_shape=[out] * 2,
        compiler_params=params(1),
        cost_estimate=pl.CostEstimate(flops=4 * n * seq * dim * dim, bytes_accessed=6 * n * seq * dim, transcendentals=0),
        name="other_kv",
    )(role, h_o, w_t, b_qkv)


def head_only(z, h, head):
    lane = lax.broadcasted_iota(jnp.int32, z.shape, 1)
    return jnp.where((lane >= h * head) & (lane < (h + 1) * head), z, jnp.zeros_like(z))


def attn_kernel(role_ref, q_ref, g_ref, k_ref, v_ref, ko_ref, vo_ref, *rest, head, scale):
    a_ref, dq_ref, dk_ref, dv_ref, dkb_ref, dvb_ref, st_ref = rest[-7:]
    seq, width = k_ref.shape[1:]
    blk = seq // 2
    causal = lax.broadcasted_iota(jnp.int32, (blk, blk), 0) <= lax.broadcasted_iota(jnp.int32, (blk, blk), 1)

    def run(rect):
        k_t, v_t = k_ref[0].T, v_ref[0].T
        if rect:
            ko_t, vo_t = ko_ref[0].T, vo_ref[0].T
        for qi in range(2):
            rows = slice(qi * blk, (qi + 1) * blk)
            near = (qi + 1) * blk
            q2 = q_ref[0, 0, rows, :] * jnp.asarray(scale, BF16)
            g2 = g_ref[0, 0, rows, :]
            o_parts, dq_parts, p_near, ds_near, q_only, g_only = [], [], [], [], [], []
            for h in range(width // head):
                hrow = slice(h * head, (h + 1) * head)
                qm, gm = head_only(q2, h, head), head_only(g2, h, head)

                def products(mine, far, z):
                    near_z = dot_nt(mine[0, :near, :], z)
                    parts = [near_z] if qi == 0 else [near_z[:blk], near_z[blk:]]
                    return parts + ([dot_nt(far[0], z)] if rect else [])

                s = products(k_ref, ko_ref, qm)
                s[qi] = jnp.where(causal, s[qi], -jnp.inf)
                m = functools.reduce(jnp.maximum, [jnp.max(s_i, axis=0, keepdims=True) for s_i in s])
                e = [jnp.exp(s_i - m) for s_i in s]
                dp = products(v_ref, vo_ref, gm)
                l = functools.reduce(jnp.add, [jnp.sum(e_i, axis=0, keepdims=True) for e_i in e])
                c = functools.reduce(jnp.add, [jnp.sum(e_i * d_i, axis=0, keepdims=True) for e_i, d_i in zip(e, dp)])
                inv_l = 1.0 / l
                c = c * inv_l
                st_ref[0, 0, 2 * h, rows] = (m + jnp.log(l))[0]
                st_ref[0, 0, 2 * h + 1, rows] = c[0]
                p = [e_i * inv_l for e_i in e]
                ds = [(p_i * (d_i - c)).astype(BF16) for p_i, d_i in zip(p, dp)]
                p = [p_i.astype(BF16) for p_i in p]
                kt_h, vt_h = k_t[hrow, :near], v_t[hrow, :near]
                if rect:
                    kt_h = jnp.concatenate([kt_h, ko_t[hrow]], axis=1)
                    vt_h = jnp.concatenate([vt_h, vo_t[hrow]], axis=1)
                o_parts.append(dot_nn(vt_h, jnp.concatenate(p, axis=0)))
                dq_parts.append(dot_nn(kt_h, jnp.concatenate(ds, axis=0)))
                p_near.append(jnp.concatenate(p[:qi + 1], axis=0))
                ds_near.append(jnp.concatenate(ds[:qi + 1], axis=0))
                q_only.append(qm)
                g_only.append(gm)
            a_ref[0, rows, :] = jnp.concatenate(o_parts, axis=0).T.astype(BF16)
            dq_ref[0, rows, :] = (jnp.concatenate(dq_parts, axis=0).T * scale).astype(BF16)
            for acc_ref, parts, other in ((dk_ref, ds_near, q_only), (dv_ref, p_near, g_only)):
                val = dot_nn(jnp.concatenate(parts, axis=1), jnp.concatenate(other, axis=0))
                if qi == 0:
                    acc_ref[0, :blk, :] = val
                else:
                    acc_ref[0, :blk, :] += val[:blk]
                    acc_ref[0, blk:, :] = val[blk:]
        if rect:
            dkb_ref[0] = dk_ref[0].astype(BF16)
            dvb_ref[0] = dv_ref[0].astype(BF16)

    pl.when(role_ref[0] == 0)(lambda: run(False))
    pl.when(role_ref[0] == 1)(lambda: run(True))


def attend(role, qd, k, v, lo, k_o, v_o, head, after):
    n, seq, dim = k_o.shape
    width = 128
    pairs = dim // width
    pick = lambda t: pl.BlockSpec((1, 1, seq, width), lambda b, p, r: (t, b + lo, 0, p))
    tok_in = pl.BlockSpec((1, seq, width), lambda b, p, r: (b + lo, 0, p))
    tok = pl.BlockSpec((1, seq, width), lambda b, p, r: (b, 0, p))
    high = pl.BlockSpec((1, seq, width), lambda b, p, r: (b * r[0], 0, p * r[0]))
    low = pl.BlockSpec((1, seq, width), lambda b, p, r: (b * (1 - r[0]), 0, p * (1 - r[0])))
    narrow = jax.ShapeDtypeStruct((n, seq, dim), BF16)
    acc = jax.ShapeDtypeStruct((n, seq, dim), F32)
    return pl.pallas_call(
        functools.partial(attn_kernel, head=head, scale=head ** -0.5),
        grid_spec=pltpu.PrefetchScalarGridSpec(
            num_scalar_prefetch=1,
            grid=(n, pairs),
            in_specs=[pick(1), pick(0), tok_in, tok_in, high, high] + [UNREAD] * len(after),
            out_specs=[tok, tok, low, low, high, high, pl.BlockSpec((1, 1, 4, seq), lambda b, p, r: (b, p, 0, 0))],
        ),
        out_shape=[narrow, narrow, acc, acc, narrow, narrow, jax.ShapeDtypeStruct((n, pairs, 4, seq), F32)],
        compiler_params=params(2),
        cost_estimate=pl.CostEstimate(flops=32 * n * seq * seq * dim, bytes_accessed=24 * n * seq * dim, transcendentals=0),
        name="attend",
    )(role, qd, qd, k, v, k_o, v_o, *after)


def late_kernel(role_ref, q_ref, g_ref, st_ref, k_ref, v_ref, dka_ref, dva_ref, dkb_ref, dvb_ref, *rest, head, scale):
    dk_ref, dv_ref = rest[-2:]
    seq, width = k_ref.shape[1:]
    blk = seq // 2

    @pl.when(role_ref[0] == 1)
    def _():
        dk_ref[0] = dkb_ref[0]
        dv_ref[0] = dvb_ref[0]

    @pl.when(role_ref[0] == 0)
    def _():
        dk, dv = dka_ref[0], dva_ref[0]
        for qi in range(2):
            rows = slice(qi * blk, (qi + 1) * blk)
            q2 = q_ref[0, 0, rows, :] * jnp.asarray(scale, BF16)
            g2 = g_ref[0, 0, rows, :]
            ps, dss, q_only, g_only = [], [], [], []
            for h in range(width // head):
                qm, gm = head_only(q2, h, head), head_only(g2, h, head)
                lse = st_ref[0, 0, 2 * h, rows].reshape(1, blk)
                c = st_ref[0, 0, 2 * h + 1, rows].reshape(1, blk)
                p = jnp.exp(dot_nt(k_ref[0], qm) - lse)
                dss.append((p * (dot_nt(v_ref[0], gm) - c)).astype(BF16))
                ps.append(p.astype(BF16))
                q_only.append(qm)
                g_only.append(gm)
            dv = dv + dot_nn(jnp.concatenate(ps, axis=1), jnp.concatenate(g_only, axis=0))
            dk = dk + dot_nn(jnp.concatenate(dss, axis=1), jnp.concatenate(q_only, axis=0))
        dk_ref[0] = dk.astype(BF16)
        dv_ref[0] = dv.astype(BF16)


def late(role, qd_o, stats, k, v, lo, dk_acc, dv_acc, dk_b, dv_b, head, after):
    n, seq, dim = dk_acc.shape
    width = 128
    pairs = dim // width
    pick = lambda t: pl.BlockSpec((1, 1, seq, width), lambda b, p, r: (t, b * (1 - r[0]), 0, p * (1 - r[0])))
    low_in = pl.BlockSpec((1, seq, width), lambda b, p, r: (lo + b * (1 - r[0]), 0, p * (1 - r[0])))
    low = pl.BlockSpec((1, seq, width), lambda b, p, r: (b * (1 - r[0]), 0, p * (1 - r[0])))
    first = pl.BlockSpec((1, seq, width), lambda b, p, r: (0, 0, 0))
    narrow = jax.ShapeDtypeStruct((n, seq, dim), BF16)
    return pl.pallas_call(
        functools.partial(late_kernel, head=head, scale=head ** -0.5),
        grid_spec=pltpu.PrefetchScalarGridSpec(
            num_scalar_prefetch=1,
            grid=(n, pairs),
            in_specs=[pick(1), pick(0), pl.BlockSpec((1, 1, 4, seq), lambda b, p, r: (b, p, 0, 0)), low_in, low_in, low, low, first, first] + [UNREAD] * len(after),
            out_specs=[low] * 2,
        ),
        out_shape=[narrow] * 2,
        input_output_aliases={8: 0, 9: 1},
        compiler_params=params(2),
        cost_estimate=pl.CostEstimate(flops=16 * n * seq * seq * dim, bytes_accessed=20 * n * seq * dim, transcendentals=0),
        name="late",
    )(role, qd_o, qd_o, stats, k, v, dk_acc, dv_acc, dk_b, dv_b, *after)


def split_rows(core_ref, full_ref, own_ref, send_ref):
    run = own_ref.shape[1]
    own_ref[0] = full_ref[pl.ds(pl.multiple_of(core_ref[0] * run, run), run), :]
    send_ref[0] = full_ref[pl.ds(pl.multiple_of((1 - core_ref[0]) * run, run), run), :]


def post_kernel(core_ref, a_ref, x_ref, wo_ref, bo_ref, *rest):
    own_ref, send_ref, full_ref = rest[-3:]
    out = dot_nn(a_ref[0], wo_ref[...]) + bo_ref[...]
    full_ref[...] = (x_ref[0].astype(F32) + out).astype(BF16)
    split_rows(core_ref, full_ref, own_ref, send_ref)


def row_outputs(batch, run, dim, first):
    own = pl.BlockSpec((1, run, dim), lambda b, c: (c[0] * (batch // 2) + first + b, 0, 0))
    other = pl.BlockSpec((1, run, dim), lambda b, c: (first + b, 0, 0))
    return [own, other], [jax.ShapeDtypeStruct((batch, run, dim), BF16), jax.ShapeDtypeStruct((batch // 2, run, dim), BF16)]


def post(core, a, x, lo, w_o, b_o, batch, first, prev):
    n, seq, dim = a.shape
    run = seq // 2
    tok = pl.BlockSpec((1, seq, dim), lambda b, c: (b, 0, 0))
    tok_in = pl.BlockSpec((1, seq, dim), lambda b, c: (b + lo, 0, 0))
    whole = lambda shape: pl.BlockSpec(shape, lambda b, c: (0,) * len(shape))
    specs, shapes = row_outputs(batch, run, dim, first)
    return pl.pallas_call(
        post_kernel,
        grid_spec=pltpu.PrefetchScalarGridSpec(
            num_scalar_prefetch=1,
            grid=(n,),
            in_specs=[tok, tok_in, whole((dim, dim)), whole((1, dim))] + [UNREAD] * len(prev),
            out_specs=specs,
            scratch_shapes=[pltpu.VMEM((seq, dim), BF16)],
        ),
        out_shape=shapes,
        input_output_aliases={5 + i: i for i in range(len(prev))},
        compiler_params=params(1),
        cost_estimate=pl.CostEstimate(flops=2 * n * seq * dim * dim, bytes_accessed=6 * n * seq * dim, transcendentals=0),
        name="post",
    )(core, a, x, w_o, b_o, *prev)


def back_kernel(core_ref, dq_ref, dk_ref, dv_ref, x_ref, g_ref, lng_ref, w_ref, prev_ref, *rest):
    own_ref, send_ref, acc_ref, full_ref = rest[-4:]
    dim = x_ref.shape[2]

    @pl.when(pl.program_id(0) == 0)
    def _():
        acc_ref[...] = prev_ref[...]

    dh = dot_nn(dq_ref[0], w_ref[0:dim, :]) + dot_nn(dk_ref[0], w_ref[dim:2 * dim, :]) + dot_nn(dv_ref[0], w_ref[2 * dim:3 * dim, :])
    x_hat, inv_std = normed(x_ref[0].astype(F32))
    g = g_ref[0].astype(F32)
    u = dh * lng_ref[...]
    dx = inv_std * (u - jnp.mean(u, axis=-1, keepdims=True) - x_hat * jnp.mean(u * x_hat, axis=-1, keepdims=True))
    full_ref[...] = (g + dx).astype(BF16)
    split_rows(core_ref, full_ref, own_ref, send_ref)
    acc_ref[0:1, :] += jnp.sum(dh * x_hat, axis=0, keepdims=True)
    acc_ref[1:2, :] += jnp.sum(dh, axis=0, keepdims=True)
    for t, ref in enumerate((dq_ref, dk_ref, dv_ref)):
        acc_ref[2 + t:3 + t, :] += jnp.sum(ref[0].astype(F32), axis=0, keepdims=True)
    acc_ref[5:6, :] += jnp.sum(g, axis=0, keepdims=True)


def back(core, dq, dk, dv, x, g, lo, ln_g, w_t, acc, batch, first, prev, after):
    n, seq, dim = dq.shape
    run = seq // 2
    tok = pl.BlockSpec((1, seq, dim), lambda b, c: (b, 0, 0))
    tok_in = pl.BlockSpec((1, seq, dim), lambda b, c: (b + lo, 0, 0))
    whole = lambda shape: pl.BlockSpec(shape, lambda b, c: (0,) * len(shape))
    specs, shapes = row_outputs(batch, run, dim, first)
    return pl.pallas_call(
        back_kernel,
        grid_spec=pltpu.PrefetchScalarGridSpec(
            num_scalar_prefetch=1,
            grid=(n,),
            in_specs=[tok] * 3 + [tok_in] * 2 + [whole((1, dim)), whole((3 * dim, dim)), whole((8, dim))] + [UNREAD] * (len(prev) + len(after)),
            out_specs=specs + [whole((8, dim))],
            scratch_shapes=[pltpu.VMEM((seq, dim), BF16)],
        ),
        out_shape=shapes + [jax.ShapeDtypeStruct((8, dim), F32)],
        input_output_aliases={9 + i: i for i in range(len(prev))},
        compiler_params=params(1),
        cost_estimate=pl.CostEstimate(flops=6 * n * seq * dim * dim, bytes_accessed=12 * n * seq * dim, transcendentals=0),
        name="back",
    )(core, dq, dk, dv, x, g, ln_g, w_t, acc, *prev, *after)


def tok_dot(a, b):
    return lax.dot_general(a, b, (((0, 1), (0, 1)), ((), ())), preferred_element_type=F32)


def solution(mesh):
    tok_spec = P('dp', 'sp', None)
    part_spec = P('dp')

    def local_step(x, g, ln_g, ln_b, w_qkv, b_qkv, w_out, b_out):
        batch, _, dim = x.shape
        _, _, heads, head = w_qkv.shape
        index = lax.axis_index('sp')
        chip, core = lax.div(index, 2), lax.rem(index, 2)
        role, side = chip.reshape(1), core.reshape(1)
        ln_g2, ln_b2, b_o = ln_g.reshape(1, dim), ln_b.reshape(1, dim), b_out.reshape(1, dim)
        w_t = jnp.transpose(w_qkv, (1, 2, 3, 0)).reshape(3 * dim, dim)
        w_o = w_out.reshape(dim, dim)
        b_all = b_qkv.reshape(1, 3 * dim)
        half_b = batch // 2
        n = half_b // CHUNKS
        half_d = dim // 2

        def send(z, perm):
            return lax.ppermute(z, 'sp', perm)

        def handed(z, lo, count):
            return send(lax.dynamic_slice_in_dim(z, (1 - core) * half_b + lo, count, 0), SWAP_CORE)

        spans = ((0, n), (n, half_b - n))
        got = [(handed(g, *span), handed(x, *span)) for span in spans]
        fronts = []
        for j, (lo, _) in enumerate(spans):
            fronts.append(front(side, x, got[j][1], g, got[j][0], ln_g2, ln_b2, w_t, b_all, w_o, lo))
        own, far = [], []
        for i in range(CHUNKS):
            group, lo = fronts[min(i, 1)], max(i - 1, 0) * n
            own.append((group, lo))
            h, qd = group[0][lo:lo + n], group[1][:, lo:lo + n]
            far.append((send(h, UP), send(qd, DOWN)))

        def halves_added(w):
            theirs = send(lax.dynamic_slice_in_dim(w, (1 - core) * half_d, half_d, 0), SWAP_CORE)
            return lax.dynamic_slice_in_dim(w, core * half_d, half_d, 0) + theirs

        att, stats = {}, {}
        dw = {}
        d_x, acc = [], jnp.zeros((8, dim), F32)

        def add_to(name, part):
            dw[name] = part if name not in dw else dw[name] + part

        def forward(i, after):
            (h, qd, k, v, xb, gb), lo = own[i]
            k_o, v_o = other_kv(role, far[i][0], w_t, b_all)
            att[i] = attend(role, qd, k, v, lo, k_o, v_o, head, after)
            stats[i] = send(att[i][6], DOWN)

        def backward(i, after, d_x, acc):
            (h, qd, k, v, xb, gb), lo = own[i]
            _, dq, dk_acc, dv_acc, dk_b, dv_b, _ = att[i]
            dk, dv = late(role, far[i][1], stats[i], k, v, lo, dk_acc, dv_acc, dk_b, dv_b, head, after)
            dwk, dwv = tok_dot(dk, h[lo:lo + n]), tok_dot(dv, h[lo:lo + n])
            add_to('k', dwk)
            add_to('v', dwv)
            after = [dwk, dwv]
            if i == CHUNKS - 1:
                after = [halves_added(dw['k']), halves_added(dw['v'])]
            *d_x, acc = back(side, dq, dk, dv, xb, gb, lo, ln_g2, w_t, acc, batch, i * n, d_x, after)
            return d_x, acc, after

        for i in range(CHUNKS - 1):
            forward(i, [])
        d_x, acc, _ = backward(0, [att[CHUNKS - 2][6]], d_x, acc)
        forward(CHUNKS - 1, [acc])
        d_x, acc, _ = backward(1, [att[CHUNKS - 1][6]], d_x, acc)
        y = []
        for i in range(CHUNKS):
            (h, qd, k, v, xb, gb), lo = own[i]
            y = post(side, att[i][0], xb, lo, w_o, b_o, batch, i * n, y)
            add_to('o', tok_dot(att[i][0], gb[lo:lo + n]))
            add_to('q', tok_dot(att[i][1], h[lo:lo + n]))
        d_x, acc, _ = backward(2, [acc, y[1]], d_x, acc)
        part_o, part_q = halves_added(dw['o']), halves_added(dw['q'])
        sum_o = part_o + send(part_o, SWAP_CHIP)
        sum_q = part_q + send(part_q, SWAP_CHIP)
        d_x, acc, (part_k, part_v) = backward(3, [acc, part_o, part_q], d_x, acc)
        sum_k = part_k + send(part_k, SWAP_CHIP)
        sum_v = part_v + send(part_v, SWAP_CHIP)

        def joined(own_rows, other_rows):
            return lax.dynamic_update_slice_in_dim(own_rows, send(other_rows, SWAP_CORE), (1 - core) * half_b, 0)

        y, d_x = joined(*y), joined(*d_x)
        acc = acc + send(acc, SWAP_CORE)
        acc = acc + send(acc, SWAP_CHIP)

        d_w_out = jnp.zeros((dim, dim), F32)
        d_w_out = lax.dynamic_update_slice(d_w_out, sum_o, (core * half_d, 0))
        d_w_out = lax.dynamic_update_slice(d_w_out, send(sum_o, SWAP_CORE), ((1 - core) * half_d, 0))
        dwt = jnp.zeros((3 * dim, dim), F32)
        for t, w in enumerate((sum_q, sum_k, sum_v)):
            dwt = lax.dynamic_update_slice(dwt, w, (t * dim + core * half_d, 0))
            dwt = lax.dynamic_update_slice(dwt, send(w, SWAP_CORE), (t * dim + (1 - core) * half_d, 0))
        d_w_qkv = jnp.transpose(dwt.reshape(3, heads, head, dim), (3, 0, 1, 2))
        return y, d_x, acc[0], acc[1], d_w_qkv, acc[2:5].reshape(3, heads, head), d_w_out.reshape(heads, head, dim), acc[5]


    return jax.shard_map(local_step, mesh=mesh, in_specs=(tok_spec, tok_spec) + (P(),) * 6, out_specs=(tok_spec, tok_spec) + (part_spec,) * 6, check_vma=False)
```

```python
import functools

import jax
import jax.numpy as jnp
from jax import lax
from jax.experimental import pallas as pl
from jax.experimental.pallas import tpu as pltpu
from jax.sharding import PartitionSpec as P


LN_EPS = 1e-5
F32 = jnp.float32
BF16 = jnp.bfloat16
CHUNKS = 4
UP = [(0, 2), (1, 3)]
DOWN = [(2, 0), (3, 1)]
SWAP_CHIP = [(0, 2), (1, 3), (2, 0), (3, 1)]
SWAP_CORE = [(0, 1), (1, 0), (2, 3), (3, 2)]


UNREAD = pl.BlockSpec(memory_space=pltpu.HBM)


def dot_nn(a, b):
    return lax.dot_general(a, b, (((1,), (0,)), ((), ())), preferred_element_type=F32)


def dot_nt(a, b):
    return lax.dot_general(a, b, (((1,), (1,)), ((), ())), preferred_element_type=F32)


def params(n):
    return pltpu.CompilerParams(dimension_semantics=("arbitrary",) * n, vmem_limit_bytes=56 * 1024 * 1024)


def normed(x_f):
    centred = x_f - jnp.mean(x_f, axis=-1, keepdims=True)
    inv_std = lax.rsqrt(jnp.mean(centred * centred, axis=-1, keepdims=True) + LN_EPS)
    return centred * inv_std, inv_std


def front_kernel(core_ref, x_ref, xr_ref, g_ref, gr_ref, lng_ref, lnb_ref, w_ref, b_ref, wo_ref,
                 *rest):
    hs_ref, qd_ref, k_ref, v_ref, h_ref, xb_ref, gb_ref = rest[-7:]
    dim = x_ref.shape[2]
    run = x_ref.shape[1]
    mine = pl.ds(pl.multiple_of(core_ref[0] * run, run), run)
    theirs = pl.ds(pl.multiple_of((1 - core_ref[0]) * run, run), run)
    xb_ref[0, mine, :] = x_ref[0]
    xb_ref[0, theirs, :] = xr_ref[0]
    gb_ref[0, mine, :] = g_ref[0]
    gb_ref[0, theirs, :] = gr_ref[0]
    qd_ref[0, 0] = dot_nt(gb_ref[0], wo_ref[...]).astype(BF16)
    x_hat, _ = normed(xb_ref[0].astype(F32))
    h_ref[0] = (x_hat * lng_ref[...] + lnb_ref[...]).astype(BF16)
    hs_ref[0] = h_ref[0]
    for t in range(3):
        cols = slice(t * dim, (t + 1) * dim)
        val = (dot_nt(h_ref[0], w_ref[cols, :]) + b_ref[:, cols]).astype(BF16)
        if t == 0:
            qd_ref[1, 0] = val
        else:
            (k_ref if t == 1 else v_ref)[0] = val


def front(core, x, x_r, g, g_r, ln_g, ln_b, w_t, b_qkv, w_o, lo, prev):
    batch, run, dim = x.shape
    n, seq = x_r.shape[0], 2 * run
    whole = lambda shape: pl.BlockSpec(shape, lambda b, c: (0,) * len(shape))
    own = pl.BlockSpec((1, run, dim), lambda b, c: (c[0] * (batch // 2) + lo + b, 0, 0))
    got = pl.BlockSpec((1, run, dim), lambda b, c: (b, 0, 0))
    tok = pl.BlockSpec((1, seq, dim), lambda b, c: (b, 0, 0))
    row = pl.BlockSpec((1, seq, dim), lambda b, c: (lo + b, 0, 0))
    out = jax.ShapeDtypeStruct((n, seq, dim), BF16)
    all_rows = jax.ShapeDtypeStruct((batch // 2, seq, dim), BF16)
    return pl.pallas_call(
        front_kernel,
        grid_spec=pltpu.PrefetchScalarGridSpec(
            num_scalar_prefetch=1,
            grid=(n,),
            in_specs=[own, got, own, got, whole((1, dim)), whole((1, dim)), whole((3 * dim, dim)), whole((1, 3 * dim)), whole((dim, dim))] + [UNREAD] * len(prev),
            out_specs=[tok, pl.BlockSpec((2, 1, seq, dim), lambda b, c: (0, b, 0, 0)), tok, tok, row, row, row],
        ),
        out_shape=[out, jax.ShapeDtypeStruct((2, n, seq, dim), BF16), out, out] + [all_rows] * 3,
        input_output_aliases={10 + i: 4 + i for i in range(len(prev))},
        compiler_params=params(1),
        cost_estimate=pl.CostEstimate(flops=8 * n * seq * dim * dim, bytes_accessed=18 * n * seq * dim, transcendentals=0),
        name="front",
    )(core, x, x_r, g, g_r, ln_g, ln_b, w_t, b_qkv, w_o, *prev)


def kv_kernel(role_ref, h_ref, wk_ref, wv_ref, b_ref, k_ref, v_ref):
    dim = h_ref.shape[2]

    @pl.when(role_ref[0] == 1)
    def _():
        for t, w_ref, out in ((1, wk_ref, k_ref), (2, wv_ref, v_ref)):
            out[0] = (dot_nt(h_ref[0], w_ref[...]) + b_ref[:, t * dim:(t + 1) * dim]).astype(BF16)


def other_kv(role, h_o, w_t, b_qkv):
    n, seq, dim = h_o.shape
    tok = pl.BlockSpec((1, seq, dim), lambda b, r: (b * r[0], 0, 0))
    third = lambda t: pl.BlockSpec((dim, dim), lambda b, r: (t, 0))
    out = jax.ShapeDtypeStruct((n, seq, dim), BF16)
    return pl.pallas_call(
        kv_kernel,
        grid_spec=pltpu.PrefetchScalarGridSpec(
            num_scalar_prefetch=1,
            grid=(n,),
            in_specs=[tok, third(1), third(2), pl.BlockSpec((1, 3 * dim), lambda b, r: (0, 0))],
            out_specs=[tok] * 2,
        ),
        out_shape=[out] * 2,
        compiler_params=params(1),
        cost_estimate=pl.CostEstimate(flops=4 * n * seq * dim * dim, bytes_accessed=6 * n * seq * dim, transcendentals=0),
        name="other_kv",
    )(role, h_o, w_t, w_t, b_qkv)


def head_only(z, h, head):
    lane = lax.broadcasted_iota(jnp.int32, z.shape, 1)
    return jnp.where((lane >= h * head) & (lane < (h + 1) * head), z, jnp.zeros_like(z))


def attn_kernel(role_ref, q_ref, g_ref, k_ref, v_ref, ko_ref, vo_ref, *rest, head, scale):
    a_ref, dq_ref, dkb_ref, dvb_ref, dk_ref, dv_ref, st_ref = rest[-7:]
    seq, width = k_ref.shape[1:]
    blk = seq // 2
    causal = lax.broadcasted_iota(jnp.int32, (blk, blk), 0) <= lax.broadcasted_iota(jnp.int32, (blk, blk), 1)

    def run(rect):
        k_t, v_t = k_ref[0].T, v_ref[0].T
        if rect:
            ko_t, vo_t = ko_ref[0].T, vo_ref[0].T
        for qi in range(2):
            rows = slice(qi * blk, (qi + 1) * blk)
            near = (qi + 1) * blk
            q2 = q_ref[0, 0, rows, :] * jnp.asarray(scale, BF16)
            g2 = g_ref[0, 0, rows, :]
            o_parts, dq_parts, p_near, ds_near, q_only, g_only = [], [], [], [], [], []
            for h in range(width // head):
                hrow = slice(h * head, (h + 1) * head)
                qm, gm = head_only(q2, h, head), head_only(g2, h, head)

                def products(mine, far, z):
                    near_z = dot_nt(mine[0, :near, :], z)
                    parts = [near_z] if qi == 0 else [near_z[:blk], near_z[blk:]]
                    return parts + ([dot_nt(far[0], z)] if rect else [])

                s = products(k_ref, ko_ref, qm)
                s[qi] = jnp.where(causal, s[qi], -jnp.inf)
                m = functools.reduce(jnp.maximum, [jnp.max(s_i, axis=0, keepdims=True) for s_i in s])
                e = [jnp.exp(s_i - m) for s_i in s]
                dp = products(v_ref, vo_ref, gm)
                l = functools.reduce(jnp.add, [jnp.sum(e_i, axis=0, keepdims=True) for e_i in e])
                c = functools.reduce(jnp.add, [jnp.sum(e_i * d_i, axis=0, keepdims=True) for e_i, d_i in zip(e, dp)])
                c = c / l
                lse = m + jnp.log(l)
                st_ref[0, 0, 2 * h, rows] = lse[0]
                st_ref[0, 0, 2 * h + 1, rows] = c[0]
                p = [jnp.exp(s_i - lse) for s_i in s]
                ds = [(p_i * (d_i - c)).astype(BF16) for p_i, d_i in zip(p, dp)]
                p = [p_i.astype(BF16) for p_i in p]
                kt_h, vt_h = k_t[hrow, :near], v_t[hrow, :near]
                if rect:
                    kt_h = jnp.concatenate([kt_h, ko_t[hrow]], axis=1)
                    vt_h = jnp.concatenate([vt_h, vo_t[hrow]], axis=1)
                o_parts.append(dot_nn(vt_h, jnp.concatenate(p, axis=0)))
                dq_parts.append(dot_nn(kt_h, jnp.concatenate(ds, axis=0)))
                p_near.append(jnp.concatenate(p[:qi + 1], axis=0))
                ds_near.append(jnp.concatenate(ds[:qi + 1], axis=0))
                q_only.append(qm)
                g_only.append(gm)
            a_ref[0, rows, :] = jnp.concatenate(o_parts, axis=0).T.astype(BF16)
            dq_ref[0, rows, :] = (jnp.concatenate(dq_parts, axis=0).T * scale).astype(BF16)
            for acc_ref, parts, other in ((dk_ref, ds_near, q_only), (dv_ref, p_near, g_only)):
                val = dot_nn(jnp.concatenate(parts, axis=1), jnp.concatenate(other, axis=0))
                if qi == 0:
                    acc_ref[0, :blk, :] = val
                else:
                    acc_ref[0, :blk, :] += val[:blk]
                    acc_ref[0, blk:, :] = val[blk:]
        if rect:
            dkb_ref[0] = dk_ref[0].astype(BF16)
            dvb_ref[0] = dv_ref[0].astype(BF16)

    pl.when(role_ref[0] == 0)(lambda: run(False))
    pl.when(role_ref[0] == 1)(lambda: run(True))


def attend(role, qd, k, v, lo, k_o, v_o, head, first, batch, prev, after):
    n, seq, dim = k_o.shape
    width = 128
    pairs = dim // width
    pick = lambda t: pl.BlockSpec((1, 1, seq, width), lambda b, p, r: (t, b + lo, 0, p))
    tok_in = pl.BlockSpec((1, seq, width), lambda b, p, r: (b + lo, 0, p))
    row = pl.BlockSpec((1, seq, width), lambda b, p, r: (first + b, 0, p))
    high_in = pl.BlockSpec((1, seq, width), lambda b, p, r: (b * r[0], 0, p * r[0]))
    high = pl.BlockSpec((1, seq, width), lambda b, p, r: (first + b * r[0], 0, p * r[0]))
    low = pl.BlockSpec((1, seq, width), lambda b, p, r: (b * (1 - r[0]), 0, p * (1 - r[0])))
    all_rows = jax.ShapeDtypeStruct((batch, seq, dim), BF16)
    acc = jax.ShapeDtypeStruct((n, seq, dim), F32)
    return pl.pallas_call(
        functools.partial(attn_kernel, head=head, scale=head ** -0.5),
        grid_spec=pltpu.PrefetchScalarGridSpec(
            num_scalar_prefetch=1,
            grid=(n, pairs),
            in_specs=[pick(1), pick(0), tok_in, tok_in, high_in, high_in] + [UNREAD] * (len(prev) + len(after)),
            out_specs=[row, row, high, high, low, low, pl.BlockSpec((1, 1, 4, seq), lambda b, p, r: (b, p, 0, 0))],
        ),
        out_shape=[all_rows] * 4 + [acc, acc, jax.ShapeDtypeStruct((n, pairs, 4, seq), F32)],
        input_output_aliases={7 + i: i for i in range(len(prev))},
        compiler_params=params(2),
        cost_estimate=pl.CostEstimate(flops=32 * n * seq * seq * dim, bytes_accessed=24 * n * seq * dim, transcendentals=0),
        name="attend",
    )(role, qd, qd, k, v, k_o, v_o, *prev, *after)


def late_kernel(role_ref, q_ref, g_ref, st_ref, k_ref, v_ref, dka_ref, dva_ref, dkb_ref, dvb_ref, *rest, head, scale):
    dk_ref, dv_ref = rest[-2:]
    seq, width = k_ref.shape[1:]
    blk = seq // 2

    @pl.when(role_ref[0] == 1)
    def _():
        dk_ref[0] = dkb_ref[0]
        dv_ref[0] = dvb_ref[0]

    @pl.when(role_ref[0] == 0)
    def _():
        dk, dv = dka_ref[0], dva_ref[0]
        for qi in range(2):
            rows = slice(qi * blk, (qi + 1) * blk)
            q2 = q_ref[0, 0, rows, :] * jnp.asarray(scale, BF16)
            g2 = g_ref[0, 0, rows, :]
            ps, dss, q_only, g_only = [], [], [], []
            for h in range(width // head):
                qm, gm = head_only(q2, h, head), head_only(g2, h, head)
                lse = st_ref[0, 0, 2 * h, rows].reshape(1, blk)
                c = st_ref[0, 0, 2 * h + 1, rows].reshape(1, blk)
                p = jnp.exp(dot_nt(k_ref[0], qm) - lse)
                dss.append((p * (dot_nt(v_ref[0], gm) - c)).astype(BF16))
                ps.append(p.astype(BF16))
                q_only.append(qm)
                g_only.append(gm)
            dv = dv + dot_nn(jnp.concatenate(ps, axis=1), jnp.concatenate(g_only, axis=0))
            dk = dk + dot_nn(jnp.concatenate(dss, axis=1), jnp.concatenate(q_only, axis=0))
        dk_ref[0] = dk.astype(BF16)
        dv_ref[0] = dv.astype(BF16)


def late(role, qd_o, stats, k, v, lo, dk_acc, dv_acc, dk_all, dv_all, head, first, after):
    n, seq, dim = dk_acc.shape
    width = 128
    pairs = dim // width
    pick = lambda t: pl.BlockSpec((1, 1, seq, width), lambda b, p, r: (t, b * (1 - r[0]), 0, p * (1 - r[0])))
    low_in = pl.BlockSpec((1, seq, width), lambda b, p, r: (lo + b * (1 - r[0]), 0, p * (1 - r[0])))
    low = pl.BlockSpec((1, seq, width), lambda b, p, r: (b * (1 - r[0]), 0, p * (1 - r[0])))
    still = pl.BlockSpec((1, seq, width), lambda b, p, r: (first, 0, 0))
    out = pl.BlockSpec((1, seq, width), lambda b, p, r: (first + b * (1 - r[0]), 0, p * (1 - r[0])))
    return pl.pallas_call(
        functools.partial(late_kernel, head=head, scale=head ** -0.5),
        grid_spec=pltpu.PrefetchScalarGridSpec(
            num_scalar_prefetch=1,
            grid=(n, pairs),
            in_specs=[pick(1), pick(0), pl.BlockSpec((1, 1, 4, seq), lambda b, p, r: (b, p, 0, 0)), low_in, low_in, low, low, still, still] + [UNREAD] * len(after),
            out_specs=[out] * 2,
        ),
        out_shape=[jax.ShapeDtypeStruct(dk_all.shape, BF16)] * 2,
        input_output_aliases={8: 0, 9: 1},
        compiler_params=params(2),
        cost_estimate=pl.CostEstimate(flops=16 * n * seq * seq * dim, bytes_accessed=20 * n * seq * dim, transcendentals=0),
        name="late",
    )(role, qd_o, qd_o, stats, k, v, dk_acc, dv_acc, dk_all, dv_all, *after)


def split_rows(core_ref, full_ref, own_ref, send_ref):
    run = own_ref.shape[1]
    own_ref[0] = full_ref[pl.ds(pl.multiple_of(core_ref[0] * run, run), run), :]
    send_ref[0] = full_ref[pl.ds(pl.multiple_of((1 - core_ref[0]) * run, run), run), :]


def post_kernel(core_ref, a_ref, x_ref, wo_ref, bo_ref, *rest):
    own_ref, send_ref, full_ref = rest[-3:]
    out = dot_nn(a_ref[0], wo_ref[...]) + bo_ref[...]
    full_ref[...] = (x_ref[0].astype(F32) + out).astype(BF16)
    split_rows(core_ref, full_ref, own_ref, send_ref)


def row_outputs(n, run, dim):
    own = pl.BlockSpec((1, run, dim), lambda b, c: (c[0] * n + b, 0, 0))
    other = pl.BlockSpec((1, run, dim), lambda b, c: (b, 0, 0))
    return [own, other], [jax.ShapeDtypeStruct((2 * n, run, dim), BF16), jax.ShapeDtypeStruct((n, run, dim), BF16)]


def post(core, a, x, w_o, b_o, after):
    n, seq, dim = a.shape
    tok = pl.BlockSpec((1, seq, dim), lambda b, c: (b, 0, 0))
    whole = lambda shape: pl.BlockSpec(shape, lambda b, c: (0,) * len(shape))
    specs, shapes = row_outputs(n, seq // 2, dim)
    return pl.pallas_call(
        post_kernel,
        grid_spec=pltpu.PrefetchScalarGridSpec(
            num_scalar_prefetch=1,
            grid=(n,),
            in_specs=[tok, tok, whole((dim, dim)), whole((1, dim))] + [UNREAD] * len(after),
            out_specs=specs,
            scratch_shapes=[pltpu.VMEM((seq, dim), BF16)],
        ),
        out_shape=shapes,
        compiler_params=params(1),
        cost_estimate=pl.CostEstimate(flops=2 * n * seq * dim * dim, bytes_accessed=6 * n * seq * dim, transcendentals=0),
        name="post",
    )(core, a, x, w_o, b_o, *after)


def back_kernel(core_ref, dq_ref, dk_ref, dv_ref, x_ref, g_ref, lng_ref, w_ref, *rest):
    own_ref, send_ref, acc_ref, full_ref = rest[-4:]
    dim = x_ref.shape[2]

    @pl.when(pl.program_id(0) == 0)
    def _():
        acc_ref[...] = jnp.zeros_like(acc_ref)

    dh = dot_nn(dq_ref[0], w_ref[0:dim, :]) + dot_nn(dk_ref[0], w_ref[dim:2 * dim, :]) + dot_nn(dv_ref[0], w_ref[2 * dim:3 * dim, :])
    x_hat, inv_std = normed(x_ref[0].astype(F32))
    g = g_ref[0].astype(F32)
    u = dh * lng_ref[...]
    dx = inv_std * (u - jnp.mean(u, axis=-1, keepdims=True) - x_hat * jnp.mean(u * x_hat, axis=-1, keepdims=True))
    full_ref[...] = (g + dx).astype(BF16)
    split_rows(core_ref, full_ref, own_ref, send_ref)
    acc_ref[0:1, :] += jnp.sum(dh * x_hat, axis=0, keepdims=True)
    acc_ref[1:2, :] += jnp.sum(dh, axis=0, keepdims=True)
    for t, ref in enumerate((dq_ref, dk_ref, dv_ref)):
        acc_ref[2 + t:3 + t, :] += jnp.sum(ref[0].astype(F32), axis=0, keepdims=True)
    acc_ref[5:6, :] += jnp.sum(g, axis=0, keepdims=True)


def back(core, dq, dk, dv, x, g, ln_g, w_t, after):
    n, seq, dim = dq.shape
    tok = pl.BlockSpec((1, seq, dim), lambda b, c: (b, 0, 0))
    whole = lambda shape: pl.BlockSpec(shape, lambda b, c: (0,) * len(shape))
    specs, shapes = row_outputs(n, seq // 2, dim)
    return pl.pallas_call(
        back_kernel,
        grid_spec=pltpu.PrefetchScalarGridSpec(
            num_scalar_prefetch=1,
            grid=(n,),
            in_specs=[tok] * 5 + [whole((1, dim)), whole((3 * dim, dim))] + [UNREAD] * len(after),
            out_specs=specs + [whole((8, dim))],
            scratch_shapes=[pltpu.VMEM((seq, dim), BF16)],
        ),
        out_shape=shapes + [jax.ShapeDtypeStruct((8, dim), F32)],
        compiler_params=params(1),
        cost_estimate=pl.CostEstimate(flops=6 * n * seq * dim * dim, bytes_accessed=12 * n * seq * dim, transcendentals=0),
        name="back",
    )(core, dq, dk, dv, x, g, ln_g, w_t, *after)


def tok_dot(a, b):
    return lax.dot_general(a, b, (((0, 1), (0, 1)), ((), ())), preferred_element_type=F32)


def solution(mesh):
    tok_spec = P('dp', 'sp', None)
    part_spec = P('dp')

    def local_step(x, g, ln_g, ln_b, w_qkv, b_qkv, w_out, b_out):
        batch, _, dim = x.shape
        _, _, heads, head = w_qkv.shape
        index = lax.axis_index('sp')
        chip, core = lax.div(index, 2), lax.rem(index, 2)
        role, side = chip.reshape(1), core.reshape(1)
        ln_g2, ln_b2, b_o = ln_g.reshape(1, dim), ln_b.reshape(1, dim), b_out.reshape(1, dim)
        w_t = jnp.transpose(w_qkv, (1, 2, 3, 0)).reshape(3 * dim, dim)
        w_o = w_out.reshape(dim, dim)
        b_all = b_qkv.reshape(1, 3 * dim)
        half_b = batch // 2
        n = half_b // CHUNKS
        half_d = dim // 2

        def send(z, perm):
            return lax.ppermute(z, 'sp', perm)

        def handed(z, lo, count):
            return send(lax.dynamic_slice_in_dim(z, (1 - core) * half_b + lo, count, 0), SWAP_CORE)

        spans = ((0, n), (n, half_b - n))
        got = [(handed(g, *span), handed(x, *span)) for span in spans]
        fronts, whole = [], []
        for j, (lo, _) in enumerate(spans):
            *group, h, xb, gb = front(side, x, got[j][1], g, got[j][0], ln_g2, ln_b2, w_t, b_all, w_o, lo, whole)
            fronts.append(group)
            whole = [h, xb, gb]
        own, far = [], []
        for i in range(CHUNKS):
            (hs, qd, k, v), lo = fronts[min(i, 1)], max(i - 1, 0) * n
            own.append((qd, k, v, lo))
            far.append((send(hs[lo:lo + n], UP), send(qd[:, lo:lo + n], DOWN)))

        def halves_added(w):
            theirs = send(lax.dynamic_slice_in_dim(w, (1 - core) * half_d, half_d, 0), SWAP_CORE)
            return lax.dynamic_slice_in_dim(w, core * half_d, half_d, 0) + theirs

        accs, stats, sent = {}, {}, {}

        def forward(i, chain):
            k_o, v_o = other_kv(role, far[i][0], w_t, b_all)
            *chain, dk_acc, dv_acc, stats[i] = attend(role, *own[i], k_o, v_o, head, i * n, half_b, chain, [])
            accs[i] = dk_acc, dv_acc
            sent[i] = send(stats[i], DOWN)
            return chain

        def backward(i, chain, after):
            a, dq, dk, dv = chain
            _, k, v, lo = own[i]
            dk, dv = late(role, far[i][1], sent[i], k, v, lo, *accs[i], dk, dv, head, i * n, after)
            return [a, dq, dk, dv]

        chain = forward(0, [])
        chain = forward(1, chain)
        chain = forward(2, chain)
        chain = backward(0, chain, [])
        chain = forward(3, chain)
        chain = backward(1, chain, [])
        dw_o, dw_q = tok_dot(chain[0], gb), tok_dot(chain[1], h)
        part_o, part_q = halves_added(dw_o), halves_added(dw_q)
        chain = backward(2, chain, [part_o, part_q])
        sum_o = part_o + send(part_o, SWAP_CHIP)
        sum_q = part_q + send(part_q, SWAP_CHIP)
        chain = backward(3, chain, [])
        a, dq, dk, dv = chain
        part_k, part_v = halves_added(tok_dot(dk, h)), halves_added(tok_dot(dv, h))
        sum_k = part_k + send(part_k, SWAP_CHIP)
        sum_v = part_v + send(part_v, SWAP_CHIP)
        y = post(side, a, xb, w_o, b_o, [part_k, part_v])
        *d_x, acc = back(side, dq, dk, dv, xb, gb, ln_g2, w_t, [part_k, part_v])

        def joined(own_rows, other_rows):
            return lax.dynamic_update_slice_in_dim(own_rows, send(other_rows, SWAP_CORE), (1 - core) * half_b, 0)

        y, d_x = joined(*y), joined(*d_x)
        acc = acc + send(acc, SWAP_CORE)
        acc = acc + send(acc, SWAP_CHIP)

        d_w_out = jnp.zeros((dim, dim), F32)
        d_w_out = lax.dynamic_update_slice(d_w_out, sum_o, (core * half_d, 0))
        d_w_out = lax.dynamic_update_slice(d_w_out, send(sum_o, SWAP_CORE), ((1 - core) * half_d, 0))
        dwt = jnp.zeros((3 * dim, dim), F32)
        for t, w in enumerate((sum_q, sum_k, sum_v)):
            dwt = lax.dynamic_update_slice(dwt, w, (t * dim + core * half_d, 0))
            dwt = lax.dynamic_update_slice(dwt, send(w, SWAP_CORE), (t * dim + (1 - core) * half_d, 0))
        d_w_qkv = jnp.transpose(dwt.reshape(3, heads, head, dim), (3, 0, 1, 2))
        return y, d_x, acc[0], acc[1], d_w_qkv, acc[2:5].reshape(3, heads, head), d_w_out.reshape(heads, head, dim), acc[5]


    return jax.shard_map(local_step, mesh=mesh, in_specs=(tok_spec, tok_spec) + (P(),) * 6, out_specs=(tok_spec, tok_spec) + (part_spec,) * 6, check_vma=False)
```

```python
import functools

import jax
import jax.numpy as jnp
from jax import lax
from jax.experimental import pallas as pl
from jax.experimental.pallas import tpu as pltpu
from jax.sharding import PartitionSpec as P


LN_EPS = 1e-5
F32 = jnp.float32
BF16 = jnp.bfloat16
CHUNKS = 4
PAIR = 128
UP = [(0, 2), (1, 3)]
DOWN = [(2, 0), (3, 1)]
SWAP_CHIP = [(0, 2), (1, 3), (2, 0), (3, 1)]
SWAP_CORE = [(0, 1), (1, 0), (2, 3), (3, 2)]


UNREAD = pl.BlockSpec(memory_space=pltpu.HBM)


def dot_nn(a, b):
    return lax.dot_general(a, b, (((1,), (0,)), ((), ())), preferred_element_type=F32)


def dot_nt(a, b):
    return lax.dot_general(a, b, (((1,), (1,)), ((), ())), preferred_element_type=F32)


def params(n):
    return pltpu.CompilerParams(dimension_semantics=("arbitrary",) * n, vmem_limit_bytes=56 * 1024 * 1024)


def normed(x_f):
    centred = x_f - jnp.mean(x_f, axis=-1, keepdims=True)
    inv_std = lax.rsqrt(jnp.mean(centred * centred, axis=-1, keepdims=True) + LN_EPS)
    return centred * inv_std, inv_std


def front_kernel(core_ref, x_ref, xr_ref, g_ref, gr_ref, lng_ref, lnb_ref, w_ref, b_ref, wo_ref,
                 *rest):
    hs_ref, qd_ref, k_ref, v_ref, h_ref, xb_ref, gb_ref = rest[-7:]
    dim = x_ref.shape[2]
    run = x_ref.shape[1]
    mine = pl.ds(pl.multiple_of(core_ref[0] * run, run), run)
    theirs = pl.ds(pl.multiple_of((1 - core_ref[0]) * run, run), run)
    xb_ref[0, mine, :] = x_ref[0]
    xb_ref[0, theirs, :] = xr_ref[0]
    gb_ref[0, mine, :] = g_ref[0]
    gb_ref[0, theirs, :] = gr_ref[0]
    qd_ref[0, 0] = dot_nt(gb_ref[0], wo_ref[...]).astype(BF16)
    x_hat, _ = normed(xb_ref[0].astype(F32))
    h_ref[0] = (x_hat * lng_ref[...] + lnb_ref[...]).astype(BF16)
    hs_ref[0] = h_ref[0]
    for t in range(3):
        cols = slice(t * dim, (t + 1) * dim)
        val = (dot_nt(h_ref[0], w_ref[cols, :]) + b_ref[:, cols]).astype(BF16)
        if t == 0:
            qd_ref[1, 0] = val
        else:
            (k_ref if t == 1 else v_ref)[0] = val


def front(core, x, x_r, g, g_r, ln_g, ln_b, w_t, b_qkv, w_o, lo, prev):
    batch, run, dim = x.shape
    n, seq = x_r.shape[0], 2 * run
    whole = lambda shape: pl.BlockSpec(shape, lambda b, c: (0,) * len(shape))
    own = pl.BlockSpec((1, run, dim), lambda b, c: (c[0] * (batch // 2) + lo + b, 0, 0))
    got = pl.BlockSpec((1, run, dim), lambda b, c: (b, 0, 0))
    tok = pl.BlockSpec((1, seq, dim), lambda b, c: (b, 0, 0))
    row = pl.BlockSpec((1, seq, dim), lambda b, c: (lo + b, 0, 0))
    out = jax.ShapeDtypeStruct((n, seq, dim), BF16)
    all_rows = jax.ShapeDtypeStruct((batch // 2, seq, dim), BF16)
    return pl.pallas_call(
        front_kernel,
        grid_spec=pltpu.PrefetchScalarGridSpec(
            num_scalar_prefetch=1,
            grid=(n,),
            in_specs=[own, got, own, got, whole((1, dim)), whole((1, dim)), whole((3 * dim, dim)), whole((1, 3 * dim)), whole((dim, dim))] + [UNREAD] * len(prev),
            out_specs=[tok, pl.BlockSpec((2, 1, seq, dim), lambda b, c: (0, b, 0, 0)), tok, tok, row, row, row],
        ),
        out_shape=[out, jax.ShapeDtypeStruct((2, n, seq, dim), BF16), out, out] + [all_rows] * 3,
        input_output_aliases={10 + i: 4 + i for i in range(len(prev))},
        compiler_params=params(1),
        cost_estimate=pl.CostEstimate(flops=8 * n * seq * dim * dim, bytes_accessed=18 * n * seq * dim, transcendentals=0),
        name="front",
    )(core, x, x_r, g, g_r, ln_g, ln_b, w_t, b_qkv, w_o, *prev)


def kv_kernel(role_ref, h_ref, wk_ref, wv_ref, b_ref, k_ref, v_ref):
    dim = h_ref.shape[2]

    @pl.when(role_ref[0] == 1)
    def _():
        for t, w_ref, out in ((1, wk_ref, k_ref), (2, wv_ref, v_ref)):
            out[0] = (dot_nt(h_ref[0], w_ref[...]) + b_ref[:, t * dim:(t + 1) * dim]).astype(BF16)


def other_kv(role, h_o, w_t, b_qkv):
    n, seq, dim = h_o.shape
    tok = pl.BlockSpec((1, seq, dim), lambda b, r: (b * r[0], 0, 0))
    third = lambda t: pl.BlockSpec((dim, dim), lambda b, r: (t, 0))
    out = jax.ShapeDtypeStruct((n, seq, dim), BF16)
    return pl.pallas_call(
        kv_kernel,
        grid_spec=pltpu.PrefetchScalarGridSpec(
            num_scalar_prefetch=1,
            grid=(n,),
            in_specs=[tok, third(1), third(2), pl.BlockSpec((1, 3 * dim), lambda b, r: (0, 0))],
            out_specs=[tok] * 2,
        ),
        out_shape=[out] * 2,
        compiler_params=params(1),
        cost_estimate=pl.CostEstimate(flops=4 * n * seq * dim * dim, bytes_accessed=6 * n * seq * dim, transcendentals=0),
        name="other_kv",
    )(role, h_o, w_t, w_t, b_qkv)


def head_only(z, h, head):
    lane = lax.broadcasted_iota(jnp.int32, z.shape, 1)
    return jnp.where((lane >= h * head) & (lane < (h + 1) * head), z, jnp.zeros_like(z))


def each_pair(body, tok_refs, st_ref):
    def step(p, carry):
        cols = pl.ds(pl.multiple_of(p * PAIR, PAIR), PAIR)
        views = [r.at[:, :, cols] if len(r.shape) == 3 else r.at[:, :, :, cols] for r in tok_refs]
        body(*views, st_ref.at[:, pl.ds(p, 1)])
        return carry

    lax.fori_loop(0, st_ref.shape[1], step, 0)


def attn_kernel(role_ref, *refs, head, scale):
    tok_refs, st_ref = refs[:6] + refs[-7:-1], refs[-1]
    pl.when(role_ref[0] == 0)(lambda: each_pair(functools.partial(attn_pair, rect=False, head=head, scale=scale), tok_refs, st_ref))
    pl.when(role_ref[0] == 1)(lambda: each_pair(functools.partial(attn_pair, rect=True, head=head, scale=scale), tok_refs, st_ref))


def attn_pair(q_ref, g_ref, k_ref, v_ref, ko_ref, vo_ref, a_ref, dq_ref, dkb_ref, dvb_ref, dk_ref, dv_ref, st_ref, *, rect, head, scale):
    seq, width = k_ref.shape[1:]
    blk = seq // 2
    causal = lax.broadcasted_iota(jnp.int32, (blk, blk), 0) <= lax.broadcasted_iota(jnp.int32, (blk, blk), 1)

    k_t, v_t = k_ref[0].T, v_ref[0].T
    if rect:
        ko_t, vo_t = ko_ref[0].T, vo_ref[0].T
    for qi in range(2):
        rows = slice(qi * blk, (qi + 1) * blk)
        near = (qi + 1) * blk
        q2 = q_ref[0, 0, rows, :] * jnp.asarray(scale, BF16)
        g2 = g_ref[0, 0, rows, :]
        o_parts, dq_parts, p_near, ds_near, q_only, g_only = [], [], [], [], [], []
        for h in range(width // head):
            hrow = slice(h * head, (h + 1) * head)
            qm, gm = head_only(q2, h, head), head_only(g2, h, head)

            def products(mine, far, z):
                near_z = dot_nt(mine[0, :near, :], z)
                parts = [near_z] if qi == 0 else [near_z[:blk], near_z[blk:]]
                return parts + ([dot_nt(far[0], z)] if rect else [])

            s = products(k_ref, ko_ref, qm)
            s[qi] = jnp.where(causal, s[qi], -jnp.inf)
            m = functools.reduce(jnp.maximum, [jnp.max(s_i, axis=0, keepdims=True) for s_i in s])
            e = [jnp.exp(s_i - m) for s_i in s]
            dp = products(v_ref, vo_ref, gm)
            l = functools.reduce(jnp.add, [jnp.sum(e_i, axis=0, keepdims=True) for e_i in e])
            c = functools.reduce(jnp.add, [jnp.sum(e_i * d_i, axis=0, keepdims=True) for e_i, d_i in zip(e, dp)])
            inv_l = 1.0 / l
            c = c * inv_l
            st_ref[0, 0, 2 * h, rows] = (m + jnp.log(l))[0]
            st_ref[0, 0, 2 * h + 1, rows] = c[0]
            p = [e_i * inv_l for e_i in e]
            ds = [(p_i * (d_i - c)).astype(BF16) for p_i, d_i in zip(p, dp)]
            p = [p_i.astype(BF16) for p_i in p]
            kt_h, vt_h = k_t[hrow, :near], v_t[hrow, :near]
            if rect:
                kt_h = jnp.concatenate([kt_h, ko_t[hrow]], axis=1)
                vt_h = jnp.concatenate([vt_h, vo_t[hrow]], axis=1)
            o_parts.append(dot_nn(vt_h, jnp.concatenate(p, axis=0)))
            dq_parts.append(dot_nn(kt_h, jnp.concatenate(ds, axis=0)))
            p_near.append(jnp.concatenate(p[:qi + 1], axis=0))
            ds_near.append(jnp.concatenate(ds[:qi + 1], axis=0))
            q_only.append(qm)
            g_only.append(gm)
        a_ref[0, rows, :] = jnp.concatenate(o_parts, axis=0).T.astype(BF16)
        dq_ref[0, rows, :] = (jnp.concatenate(dq_parts, axis=0).T * scale).astype(BF16)
        for acc_ref, parts, other in ((dk_ref, ds_near, q_only), (dv_ref, p_near, g_only)):
            val = dot_nn(jnp.concatenate(parts, axis=1), jnp.concatenate(other, axis=0))
            if qi == 0:
                acc_ref[0, :blk, :] = val
            else:
                acc_ref[0, :blk, :] += val[:blk]
                acc_ref[0, blk:, :] = val[blk:]
    if rect:
        dkb_ref[0] = dk_ref[0].astype(BF16)
        dvb_ref[0] = dv_ref[0].astype(BF16)


def attend(role, qd, k, v, lo, k_o, v_o, head, first, batch, prev, after):
    n, seq, dim = k_o.shape
    pairs = dim // PAIR
    pick = lambda t: pl.BlockSpec((1, 1, seq, dim), lambda b, r: (t, b + lo, 0, 0))
    tok_in = pl.BlockSpec((1, seq, dim), lambda b, r: (b + lo, 0, 0))
    row = pl.BlockSpec((1, seq, dim), lambda b, r: (first + b, 0, 0))
    high_in = pl.BlockSpec((1, seq, dim), lambda b, r: (b * r[0], 0, 0))
    high = pl.BlockSpec((1, seq, dim), lambda b, r: (first + b * r[0], 0, 0))
    low = pl.BlockSpec((1, seq, dim), lambda b, r: (b * (1 - r[0]), 0, 0))
    all_rows = jax.ShapeDtypeStruct((batch, seq, dim), BF16)
    acc = jax.ShapeDtypeStruct((n, seq, dim), F32)
    return pl.pallas_call(
        functools.partial(attn_kernel, head=head, scale=head ** -0.5),
        grid_spec=pltpu.PrefetchScalarGridSpec(
            num_scalar_prefetch=1,
            grid=(n,),
            in_specs=[pick(1), pick(0), tok_in, tok_in, high_in, high_in] + [UNREAD] * (len(prev) + len(after)),
            out_specs=[row, row, high, high, low, low, pl.BlockSpec((1, pairs, 4, seq), lambda b, r: (b, 0, 0, 0))],
        ),
        out_shape=[all_rows] * 4 + [acc, acc, jax.ShapeDtypeStruct((n, pairs, 4, seq), F32)],
        input_output_aliases={7 + i: i for i in range(len(prev))},
        compiler_params=params(1),
        cost_estimate=pl.CostEstimate(flops=32 * n * seq * seq * dim, bytes_accessed=24 * n * seq * dim, transcendentals=0),
        name="attend",
    )(role, qd, qd, k, v, k_o, v_o, *prev, *after)


def late_kernel(role_ref, q_ref, g_ref, st_ref, k_ref, v_ref, dka_ref, dva_ref, dkb_ref, dvb_ref, *rest, head, scale):
    dk_ref, dv_ref = rest[-2:]

    @pl.when(role_ref[0] == 1)
    def _():
        dk_ref[0] = dkb_ref[0]
        dv_ref[0] = dvb_ref[0]

    @pl.when(role_ref[0] == 0)
    def _():
        each_pair(functools.partial(late_pair, head=head, scale=scale), (q_ref, g_ref, k_ref, v_ref, dka_ref, dva_ref, dk_ref, dv_ref), st_ref)


def late_pair(q_ref, g_ref, k_ref, v_ref, dka_ref, dva_ref, dk_ref, dv_ref, st_ref, *, head, scale):
    seq, width = k_ref.shape[1:]
    blk = seq // 2
    k, v = k_ref[0], v_ref[0]
    dk, dv = dka_ref[0], dva_ref[0]
    for qi in range(2):
        rows = slice(qi * blk, (qi + 1) * blk)
        q2 = q_ref[0, 0, rows, :] * jnp.asarray(scale, BF16)
        g2 = g_ref[0, 0, rows, :]
        ps, dss, q_only, g_only = [], [], [], []
        for h in range(width // head):
            qm, gm = head_only(q2, h, head), head_only(g2, h, head)
            lse = st_ref[0, 0, 2 * h, rows].reshape(1, blk)
            c = st_ref[0, 0, 2 * h + 1, rows].reshape(1, blk)
            p = jnp.exp(dot_nt(k, qm) - lse)
            dss.append((p * (dot_nt(v, gm) - c)).astype(BF16))
            ps.append(p.astype(BF16))
            q_only.append(qm)
            g_only.append(gm)
        dv = dv + dot_nn(jnp.concatenate(ps, axis=1), jnp.concatenate(g_only, axis=0))
        dk = dk + dot_nn(jnp.concatenate(dss, axis=1), jnp.concatenate(q_only, axis=0))
    dk_ref[0] = dk.astype(BF16)
    dv_ref[0] = dv.astype(BF16)


def late(role, qd_o, stats, k, v, lo, dk_acc, dv_acc, dk_all, dv_all, head, first, after):
    n, seq, dim = dk_acc.shape
    pairs = dim // PAIR
    pick = lambda t: pl.BlockSpec((1, 1, seq, dim), lambda b, r: (t, b * (1 - r[0]), 0, 0))
    low_in = pl.BlockSpec((1, seq, dim), lambda b, r: (lo + b * (1 - r[0]), 0, 0))
    low = pl.BlockSpec((1, seq, dim), lambda b, r: (b * (1 - r[0]), 0, 0))
    still = pl.BlockSpec((1, seq, dim), lambda b, r: (first, 0, 0))
    out = pl.BlockSpec((1, seq, dim), lambda b, r: (first + b * (1 - r[0]), 0, 0))
    stat = pl.BlockSpec((1, pairs, 4, seq), lambda b, r: (b * (1 - r[0]), 0, 0, 0))
    return pl.pallas_call(
        functools.partial(late_kernel, head=head, scale=head ** -0.5),
        grid_spec=pltpu.PrefetchScalarGridSpec(
            num_scalar_prefetch=1,
            grid=(n,),
            in_specs=[pick(1), pick(0), stat, low_in, low_in, low, low, still, still] + [UNREAD] * len(after),
            out_specs=[out] * 2,
        ),
        out_shape=[jax.ShapeDtypeStruct(dk_all.shape, BF16)] * 2,
        input_output_aliases={8: 0, 9: 1},
        compiler_params=params(1),
        cost_estimate=pl.CostEstimate(flops=16 * n * seq * seq * dim, bytes_accessed=20 * n * seq * dim, transcendentals=0),
        name="late",
    )(role, qd_o, qd_o, stats, k, v, dk_acc, dv_acc, dk_all, dv_all, *after)


def split_rows(core_ref, full_ref, own_ref, send_ref):
    run = own_ref.shape[1]
    own_ref[0] = full_ref[pl.ds(pl.multiple_of(core_ref[0] * run, run), run), :]
    send_ref[0] = full_ref[pl.ds(pl.multiple_of((1 - core_ref[0]) * run, run), run), :]


def post_kernel(core_ref, a_ref, x_ref, wo_ref, bo_ref, *rest):
    own_ref, send_ref, full_ref = rest[-3:]
    out = dot_nn(a_ref[0], wo_ref[...]) + bo_ref[...]
    full_ref[...] = (x_ref[0].astype(F32) + out).astype(BF16)
    split_rows(core_ref, full_ref, own_ref, send_ref)


def row_outputs(n, run, dim):
    own = pl.BlockSpec((1, run, dim), lambda b, c: (c[0] * n + b, 0, 0))
    other = pl.BlockSpec((1, run, dim), lambda b, c: (b, 0, 0))
    return [own, other], [jax.ShapeDtypeStruct((2 * n, run, dim), BF16), jax.ShapeDtypeStruct((n, run, dim), BF16)]


def post(core, a, x, w_o, b_o, after):
    n, seq, dim = a.shape
    tok = pl.BlockSpec((1, seq, dim), lambda b, c: (b, 0, 0))
    whole = lambda shape: pl.BlockSpec(shape, lambda b, c: (0,) * len(shape))
    specs, shapes = row_outputs(n, seq // 2, dim)
    return pl.pallas_call(
        post_kernel,
        grid_spec=pltpu.PrefetchScalarGridSpec(
            num_scalar_prefetch=1,
            grid=(n,),
            in_specs=[tok, tok, whole((dim, dim)), whole((1, dim))] + [UNREAD] * len(after),
            out_specs=specs,
            scratch_shapes=[pltpu.VMEM((seq, dim), BF16)],
        ),
        out_shape=shapes,
        compiler_params=params(1),
        cost_estimate=pl.CostEstimate(flops=2 * n * seq * dim * dim, bytes_accessed=6 * n * seq * dim, transcendentals=0),
        name="post",
    )(core, a, x, w_o, b_o, *after)


def back_kernel(core_ref, dq_ref, dk_ref, dv_ref, x_ref, g_ref, lng_ref, w_ref, *rest):
    own_ref, send_ref, acc_ref, full_ref = rest[-4:]
    dim = x_ref.shape[2]

    @pl.when(pl.program_id(0) == 0)
    def _():
        acc_ref[...] = jnp.zeros_like(acc_ref)

    dh = dot_nn(dq_ref[0], w_ref[0:dim, :]) + dot_nn(dk_ref[0], w_ref[dim:2 * dim, :]) + dot_nn(dv_ref[0], w_ref[2 * dim:3 * dim, :])
    x_hat, inv_std = normed(x_ref[0].astype(F32))
    g = g_ref[0].astype(F32)
    u = dh * lng_ref[...]
    dx = inv_std * (u - jnp.mean(u, axis=-1, keepdims=True) - x_hat * jnp.mean(u * x_hat, axis=-1, keepdims=True))
    full_ref[...] = (g + dx).astype(BF16)
    split_rows(core_ref, full_ref, own_ref, send_ref)
    acc_ref[0:1, :] += jnp.sum(dh * x_hat, axis=0, keepdims=True)
    acc_ref[1:2, :] += jnp.sum(dh, axis=0, keepdims=True)
    for t, ref in enumerate((dq_ref, dk_ref, dv_ref)):
        acc_ref[2 + t:3 + t, :] += jnp.sum(ref[0].astype(F32), axis=0, keepdims=True)
    acc_ref[5:6, :] += jnp.sum(g, axis=0, keepdims=True)


def back(core, dq, dk, dv, x, g, ln_g, w_t, after):
    n, seq, dim = dq.shape
    tok = pl.BlockSpec((1, seq, dim), lambda b, c: (b, 0, 0))
    whole = lambda shape: pl.BlockSpec(shape, lambda b, c: (0,) * len(shape))
    specs, shapes = row_outputs(n, seq // 2, dim)
    return pl.pallas_call(
        back_kernel,
        grid_spec=pltpu.PrefetchScalarGridSpec(
            num_scalar_prefetch=1,
            grid=(n,),
            in_specs=[tok] * 5 + [whole((1, dim)), whole((3 * dim, dim))] + [UNREAD] * len(after),
            out_specs=specs + [whole((8, dim))],
            scratch_shapes=[pltpu.VMEM((seq, dim), BF16)],
        ),
        out_shape=shapes + [jax.ShapeDtypeStruct((8, dim), F32)],
        compiler_params=params(1),
        cost_estimate=pl.CostEstimate(flops=6 * n * seq * dim * dim, bytes_accessed=12 * n * seq * dim, transcendentals=0),
        name="back",
    )(core, dq, dk, dv, x, g, ln_g, w_t, *after)


def join_kernel(core_ref, *refs):
    own, other, (three_ref, one_ref) = refs[:4], refs[4:8], refs[8:]

    def put(parts):
        for t in range(3):
            three_ref[t, 0] = parts[t][...]
        one_ref[0] = parts[3][...]

    pl.when(pl.program_id(0) == 0)(lambda: put(own))
    pl.when(pl.program_id(0) == 1)(lambda: put(other))


def join(core, own, other):
    half, dim = own[0].shape
    rows = 128
    steps = half // rows
    mine = pl.BlockSpec((rows, dim), lambda j, r, c: (r * (1 - j) + (steps - 1) * j, 0))
    theirs = pl.BlockSpec((rows, dim), lambda j, r, c: (r * j, 0))
    side = lambda j, c: c[0] * (1 - j) + (1 - c[0]) * j
    three, one = pl.pallas_call(
        join_kernel,
        grid_spec=pltpu.PrefetchScalarGridSpec(
            num_scalar_prefetch=1,
            grid=(2, steps),
            in_specs=[mine] * 4 + [theirs] * 4,
            out_specs=[
                pl.BlockSpec((3, 1, rows, dim), lambda j, r, c: (0, side(j, c), r, 0)),
                pl.BlockSpec((1, rows, dim), lambda j, r, c: (side(j, c), r, 0)),
            ],
        ),
        out_shape=[jax.ShapeDtypeStruct((3, 2, half, dim), F32), jax.ShapeDtypeStruct((2, half, dim), F32)],
        compiler_params=params(2),
        cost_estimate=pl.CostEstimate(flops=8 * half * dim, bytes_accessed=64 * half * dim, transcendentals=0),
        name="join",
    )(core, *own, *other)
    return three.reshape(6 * half, dim), one.reshape(2 * half, dim)


def tok_dot(a, b):
    return lax.dot_general(a, b, (((0, 1), (0, 1)), ((), ())), preferred_element_type=F32)


def solution(mesh):
    tok_spec = P('dp', 'sp', None)
    part_spec = P('dp')

    def local_step(x, g, ln_g, ln_b, w_qkv, b_qkv, w_out, b_out):
        batch, _, dim = x.shape
        _, _, heads, head = w_qkv.shape
        index = lax.axis_index('sp')
        chip, core = lax.div(index, 2), lax.rem(index, 2)
        role, side = chip.reshape(1), core.reshape(1)
        ln_g2, ln_b2, b_o = ln_g.reshape(1, dim), ln_b.reshape(1, dim), b_out.reshape(1, dim)
        w_t = jnp.transpose(w_qkv, (1, 2, 3, 0)).reshape(3 * dim, dim)
        w_o = w_out.reshape(dim, dim)
        b_all = b_qkv.reshape(1, 3 * dim)
        half_b = batch // 2
        n = half_b // CHUNKS
        half_d = dim // 2

        def send(z, perm):
            return lax.ppermute(z, 'sp', perm)

        def handed(z, lo, count):
            return send(lax.dynamic_slice_in_dim(z, (1 - core) * half_b + lo, count, 0), SWAP_CORE)

        spans = ((0, n), (n, half_b - n))
        got = [(handed(g, *span), handed(x, *span)) for span in spans]
        fronts, whole = [], []
        for j, (lo, _) in enumerate(spans):
            *group, h, xb, gb = front(side, x, got[j][1], g, got[j][0], ln_g2, ln_b2, w_t, b_all, w_o, lo, whole)
            fronts.append(group)
            whole = [h, xb, gb]
        own, far = [], []
        for i in range(CHUNKS):
            (hs, qd, k, v), lo = fronts[min(i, 1)], max(i - 1, 0) * n
            own.append((qd, k, v, lo))
            far.append((send(hs[lo:lo + n], UP), send(qd[:, lo:lo + n], DOWN)))

        def halves_added(w):
            theirs = send(lax.dynamic_slice_in_dim(w, (1 - core) * half_d, half_d, 0), SWAP_CORE)
            return lax.dynamic_slice_in_dim(w, core * half_d, half_d, 0) + theirs

        accs, stats, sent = {}, {}, {}

        def forward(i, chain):
            k_o, v_o = other_kv(role, far[i][0], w_t, b_all)
            *chain, dk_acc, dv_acc, stats[i] = attend(role, *own[i], k_o, v_o, head, i * n, half_b, chain, [])
            accs[i] = dk_acc, dv_acc
            sent[i] = send(stats[i], DOWN)
            return chain

        def backward(i, chain, after):
            a, dq, dk, dv = chain
            _, k, v, lo = own[i]
            dk, dv = late(role, far[i][1], sent[i], k, v, lo, *accs[i], dk, dv, head, i * n, after)
            return [a, dq, dk, dv]

        chain = forward(0, [])
        chain = forward(1, chain)
        chain = forward(2, chain)
        chain = backward(0, chain, [])
        chain = forward(3, chain)
        chain = backward(1, chain, [])
        dw_o, dw_q = tok_dot(chain[0], gb), tok_dot(chain[1], h)
        part_o, part_q = halves_added(dw_o), halves_added(dw_q)
        chain = backward(2, chain, [part_o, part_q])
        sum_o = part_o + send(part_o, SWAP_CHIP)
        sum_q = part_q + send(part_q, SWAP_CHIP)
        chain = backward(3, chain, [])
        a, dq, dk, dv = chain
        part_k, part_v = halves_added(tok_dot(dk, h)), halves_added(tok_dot(dv, h))
        sum_k = part_k + send(part_k, SWAP_CHIP)
        sum_v = part_v + send(part_v, SWAP_CHIP)
        y = post(side, a, xb, w_o, b_o, [part_k, part_v])
        *d_x, acc = back(side, dq, dk, dv, xb, gb, ln_g2, w_t, [part_k, part_v])

        def joined(own_rows, other_rows):
            return lax.dynamic_update_slice_in_dim(own_rows, send(other_rows, SWAP_CORE), (1 - core) * half_b, 0)

        y, d_x = joined(*y), joined(*d_x)
        acc = acc + send(acc, SWAP_CORE)
        acc = acc + send(acc, SWAP_CHIP)

        sums = (sum_q, sum_k, sum_v, sum_o)
        dwt, d_w_out = join(side, sums, [send(w, SWAP_CORE) for w in sums])
        d_w_qkv = jnp.transpose(dwt.reshape(3, heads, head, dim), (3, 0, 1, 2))
        return y, d_x, acc[0], acc[1], d_w_qkv, acc[2:5].reshape(3, heads, head), d_w_out.reshape(heads, head, dim), acc[5]


    return jax.shard_map(local_step, mesh=mesh, in_specs=(tok_spec, tok_spec) + (P(),) * 6, out_specs=(tok_spec, tok_spec) + (part_spec,) * 6, check_vma=False)
```

```python
import functools

import jax
import jax.numpy as jnp
from jax import lax
from jax.experimental import pallas as pl
from jax.experimental.pallas import tpu as pltpu
from jax.sharding import PartitionSpec as P


LN_EPS = 1e-5
F32 = jnp.float32
BF16 = jnp.bfloat16
CHUNKS = 4
PAIR = 128
UP = [(0, 2), (1, 3)]
DOWN = [(2, 0), (3, 1)]
SWAP_CHIP = [(0, 2), (1, 3), (2, 0), (3, 1)]
SWAP_CORE = [(0, 1), (1, 0), (2, 3), (3, 2)]


UNREAD = pl.BlockSpec(memory_space=pltpu.HBM)


def dot_nn(a, b):
    return lax.dot_general(a, b, (((1,), (0,)), ((), ())), preferred_element_type=F32)


def dot_nt(a, b):
    return lax.dot_general(a, b, (((1,), (1,)), ((), ())), preferred_element_type=F32)


def params(n):
    return pltpu.CompilerParams(dimension_semantics=("arbitrary",) * n, vmem_limit_bytes=56 * 1024 * 1024)


def normed(x_f):
    centred = x_f - jnp.mean(x_f, axis=-1, keepdims=True)
    inv_std = lax.rsqrt(jnp.mean(centred * centred, axis=-1, keepdims=True) + LN_EPS)
    return centred * inv_std, inv_std


def front_kernel(core_ref, x_ref, xr_ref, g_ref, gr_ref, lng_ref, lnb_ref, w_ref, b_ref, wo_ref,
                 *rest):
    hs_ref, qd_ref, k_ref, v_ref, h_ref, xb_ref, gb_ref = rest[-7:]
    dim = x_ref.shape[2]
    run = x_ref.shape[1]
    mine = pl.ds(pl.multiple_of(core_ref[0] * run, run), run)
    theirs = pl.ds(pl.multiple_of((1 - core_ref[0]) * run, run), run)
    xb_ref[0, mine, :] = x_ref[0]
    xb_ref[0, theirs, :] = xr_ref[0]
    gb_ref[0, mine, :] = g_ref[0]
    gb_ref[0, theirs, :] = gr_ref[0]
    qd_ref[0, 0] = dot_nt(gb_ref[0], wo_ref[...]).astype(BF16)
    x_hat, _ = normed(xb_ref[0].astype(F32))
    h_ref[0] = (x_hat * lng_ref[...] + lnb_ref[...]).astype(BF16)
    hs_ref[0] = h_ref[0]
    for t in range(3):
        cols = slice(t * dim, (t + 1) * dim)
        val = (dot_nt(h_ref[0], w_ref[cols, :]) + b_ref[:, cols]).astype(BF16)
        if t == 0:
            qd_ref[1, 0] = val
        else:
            (k_ref if t == 1 else v_ref)[0] = val


def front(core, x, x_r, g, g_r, ln_g, ln_b, w_t, b_qkv, w_o, lo, prev):
    batch, run, dim = x.shape
    n, seq = x_r.shape[0], 2 * run
    whole = lambda shape: pl.BlockSpec(shape, lambda b, c: (0,) * len(shape))
    own = pl.BlockSpec((1, run, dim), lambda b, c: (c[0] * (batch // 2) + lo + b, 0, 0))
    got = pl.BlockSpec((1, run, dim), lambda b, c: (b, 0, 0))
    tok = pl.BlockSpec((1, seq, dim), lambda b, c: (b, 0, 0))
    row = pl.BlockSpec((1, seq, dim), lambda b, c: (lo + b, 0, 0))
    out = jax.ShapeDtypeStruct((n, seq, dim), BF16)
    all_rows = jax.ShapeDtypeStruct((batch // 2, seq, dim), BF16)
    return pl.pallas_call(
        front_kernel,
        grid_spec=pltpu.PrefetchScalarGridSpec(
            num_scalar_prefetch=1,
            grid=(n,),
            in_specs=[own, got, own, got, whole((1, dim)), whole((1, dim)), whole((3 * dim, dim)), whole((1, 3 * dim)), whole((dim, dim))] + [UNREAD] * len(prev),
            out_specs=[tok, pl.BlockSpec((2, 1, seq, dim), lambda b, c: (0, b, 0, 0)), tok, tok, row, row, row],
        ),
        out_shape=[out, jax.ShapeDtypeStruct((2, n, seq, dim), BF16), out, out] + [all_rows] * 3,
        input_output_aliases={10 + i: 4 + i for i in range(len(prev))},
        compiler_params=params(1),
        cost_estimate=pl.CostEstimate(flops=8 * n * seq * dim * dim, bytes_accessed=18 * n * seq * dim, transcendentals=0),
        name="front",
    )(core, x, x_r, g, g_r, ln_g, ln_b, w_t, b_qkv, w_o, *prev)


def kv_kernel(role_ref, h_ref, wk_ref, wv_ref, b_ref, k_ref, v_ref):
    dim = h_ref.shape[2]

    @pl.when(role_ref[0] == 1)
    def _():
        for t, w_ref, out in ((1, wk_ref, k_ref), (2, wv_ref, v_ref)):
            out[0] = (dot_nt(h_ref[0], w_ref[...]) + b_ref[:, t * dim:(t + 1) * dim]).astype(BF16)


def other_kv(role, h_o, w_t, b_qkv):
    n, seq, dim = h_o.shape
    tok = pl.BlockSpec((1, seq, dim), lambda b, r: (b * r[0], 0, 0))
    third = lambda t: pl.BlockSpec((dim, dim), lambda b, r: (t, 0))
    out = jax.ShapeDtypeStruct((n, seq, dim), BF16)
    return pl.pallas_call(
        kv_kernel,
        grid_spec=pltpu.PrefetchScalarGridSpec(
            num_scalar_prefetch=1,
            grid=(n,),
            in_specs=[tok, third(1), third(2), pl.BlockSpec((1, 3 * dim), lambda b, r: (0, 0))],
            out_specs=[tok] * 2,
        ),
        out_shape=[out] * 2,
        compiler_params=params(1),
        cost_estimate=pl.CostEstimate(flops=4 * n * seq * dim * dim, bytes_accessed=6 * n * seq * dim, transcendentals=0),
        name="other_kv",
    )(role, h_o, w_t, w_t, b_qkv)


def head_only(z, h, head):
    lane = lax.broadcasted_iota(jnp.int32, z.shape, 1)
    return jnp.where((lane >= h * head) & (lane < (h + 1) * head), z, jnp.zeros_like(z))


def each_pair(body, tok_refs, st_ref):
    def step(p, carry):
        cols = pl.ds(pl.multiple_of(p * PAIR, PAIR), PAIR)
        views = [r.at[:, :, cols] if len(r.shape) == 3 else r.at[:, :, :, cols] for r in tok_refs]
        body(*views, st_ref.at[:, pl.ds(p, 1)])
        return carry

    lax.fori_loop(0, st_ref.shape[1], step, 0)


def attn_kernel(role_ref, *refs, head, scale):
    tok_refs, st_ref = refs[:6] + refs[-7:-1], refs[-1]
    pl.when(role_ref[0] == 0)(lambda: each_pair(functools.partial(attn_pair, rect=False, head=head, scale=scale), tok_refs, st_ref))
    pl.when(role_ref[0] == 1)(lambda: each_pair(functools.partial(attn_pair, rect=True, head=head, scale=scale), tok_refs, st_ref))


def attn_pair(q_ref, g_ref, k_ref, v_ref, ko_ref, vo_ref, a_ref, dq_ref, dkb_ref, dvb_ref, dk_ref, dv_ref, st_ref, *, rect, head, scale):
    seq, width = k_ref.shape[1:]
    blk = seq // 2
    causal = lax.broadcasted_iota(jnp.int32, (blk, blk), 0) <= lax.broadcasted_iota(jnp.int32, (blk, blk), 1)

    k_t, v_t = k_ref[0].T, v_ref[0].T
    if rect:
        ko_t, vo_t = ko_ref[0].T, vo_ref[0].T
    for qi in range(2):
        rows = slice(qi * blk, (qi + 1) * blk)
        near = (qi + 1) * blk
        q2 = q_ref[0, 0, rows, :] * jnp.asarray(scale, BF16)
        g2 = g_ref[0, 0, rows, :]
        o_parts, dq_parts, p_near, ds_near, q_only, g_only = [], [], [], [], [], []
        for h in range(width // head):
            hrow = slice(h * head, (h + 1) * head)
            qm, gm = head_only(q2, h, head), head_only(g2, h, head)

            def products(mine, far, z):
                near_z = dot_nt(mine[0, :near, :], z)
                parts = [near_z] if qi == 0 else [near_z[:blk], near_z[blk:]]
                return parts + ([dot_nt(far[0], z)] if rect else [])

            s = products(k_ref, ko_ref, qm)
            s[qi] = jnp.where(causal, s[qi], -jnp.inf)
            m = functools.reduce(jnp.maximum, [jnp.max(s_i, axis=0, keepdims=True) for s_i in s])
            e = [jnp.exp(s_i - m) for s_i in s]
            dp = products(v_ref, vo_ref, gm)
            l = functools.reduce(jnp.add, [jnp.sum(e_i, axis=0, keepdims=True) for e_i in e])
            c = functools.reduce(jnp.add, [jnp.sum(e_i * d_i, axis=0, keepdims=True) for e_i, d_i in zip(e, dp)])
            inv_l = 1.0 / l
            c = c * inv_l
            st_ref[0, 0, 2 * h, rows] = (m + jnp.log(l))[0]
            st_ref[0, 0, 2 * h + 1, rows] = c[0]
            p = [e_i * inv_l for e_i in e]
            ds = [(p_i * (d_i - c)).astype(BF16) for p_i, d_i in zip(p, dp)]
            p = [p_i.astype(BF16) for p_i in p]
            kt_h, vt_h = k_t[hrow, :near], v_t[hrow, :near]
            if rect:
                kt_h = jnp.concatenate([kt_h, ko_t[hrow]], axis=1)
                vt_h = jnp.concatenate([vt_h, vo_t[hrow]], axis=1)
            o_parts.append(dot_nn(vt_h, jnp.concatenate(p, axis=0)))
            dq_parts.append(dot_nn(kt_h, jnp.concatenate(ds, axis=0)))
            p_near.append(jnp.concatenate(p[:qi + 1], axis=0))
            ds_near.append(jnp.concatenate(ds[:qi + 1], axis=0))
            q_only.append(qm)
            g_only.append(gm)
        a_ref[0, rows, :] = jnp.concatenate(o_parts, axis=0).T.astype(BF16)
        dq_ref[0, rows, :] = (jnp.concatenate(dq_parts, axis=0).T * scale).astype(BF16)
        for acc_ref, parts, other in ((dk_ref, ds_near, q_only), (dv_ref, p_near, g_only)):
            val = dot_nn(jnp.concatenate(parts, axis=1), jnp.concatenate(other, axis=0))
            if qi == 0:
                acc_ref[0, :blk, :] = val
            else:
                acc_ref[0, :blk, :] += val[:blk]
                acc_ref[0, blk:, :] = val[blk:]
    if rect:
        dkb_ref[0] = dk_ref[0].astype(BF16)
        dvb_ref[0] = dv_ref[0].astype(BF16)


def attend(role, qd, k, v, lo, k_o, v_o, head, first, batch, prev, after):
    n, seq, dim = k_o.shape
    pairs = dim // PAIR
    pick = lambda t: pl.BlockSpec((1, 1, seq, dim), lambda b, r: (t, b + lo, 0, 0))
    tok_in = pl.BlockSpec((1, seq, dim), lambda b, r: (b + lo, 0, 0))
    row = pl.BlockSpec((1, seq, dim), lambda b, r: (first + b, 0, 0))
    high_in = pl.BlockSpec((1, seq, dim), lambda b, r: (b * r[0], 0, 0))
    high = pl.BlockSpec((1, seq, dim), lambda b, r: (first + b * r[0], 0, 0))
    low = pl.BlockSpec((1, seq, dim), lambda b, r: (b * (1 - r[0]), 0, 0))
    all_rows = jax.ShapeDtypeStruct((batch, seq, dim), BF16)
    acc = jax.ShapeDtypeStruct((n, seq, dim), F32)
    return pl.pallas_call(
        functools.partial(attn_kernel, head=head, scale=head ** -0.5),
        grid_spec=pltpu.PrefetchScalarGridSpec(
            num_scalar_prefetch=1,
            grid=(n,),
            in_specs=[pick(1), pick(0), tok_in, tok_in, high_in, high_in] + [UNREAD] * (len(prev) + len(after)),
            out_specs=[row, row, high, high, low, low, pl.BlockSpec((1, pairs, 4, seq), lambda b, r: (b, 0, 0, 0))],
        ),
        out_shape=[all_rows] * 4 + [acc, acc, jax.ShapeDtypeStruct((n, pairs, 4, seq), F32)],
        input_output_aliases={7 + i: i for i in range(len(prev))},
        compiler_params=params(1),
        cost_estimate=pl.CostEstimate(flops=32 * n * seq * seq * dim, bytes_accessed=24 * n * seq * dim, transcendentals=0),
        name="attend",
    )(role, qd, qd, k, v, k_o, v_o, *prev, *after)


def late_kernel(role_ref, q_ref, g_ref, st_ref, k_ref, v_ref, dka_ref, dva_ref, dkb_ref, dvb_ref, *rest, head, scale):
    dk_ref, dv_ref = rest[-2:]

    @pl.when(role_ref[0] == 1)
    def _():
        dk_ref[0] = dkb_ref[0]
        dv_ref[0] = dvb_ref[0]

    @pl.when(role_ref[0] == 0)
    def _():
        each_pair(functools.partial(late_pair, head=head, scale=scale), (q_ref, g_ref, k_ref, v_ref, dka_ref, dva_ref, dk_ref, dv_ref), st_ref)


def late_pair(q_ref, g_ref, k_ref, v_ref, dka_ref, dva_ref, dk_ref, dv_ref, st_ref, *, head, scale):
    seq, width = k_ref.shape[1:]
    blk = seq // 2
    k, v = k_ref[0], v_ref[0]
    dk, dv = dka_ref[0], dva_ref[0]
    for qi in range(2):
        rows = slice(qi * blk, (qi + 1) * blk)
        q2 = q_ref[0, 0, rows, :] * jnp.asarray(scale, BF16)
        g2 = g_ref[0, 0, rows, :]
        ps, dss, q_only, g_only = [], [], [], []
        for h in range(width // head):
            qm, gm = head_only(q2, h, head), head_only(g2, h, head)
            lse = st_ref[0, 0, 2 * h, rows].reshape(1, blk)
            c = st_ref[0, 0, 2 * h + 1, rows].reshape(1, blk)
            p = jnp.exp(dot_nt(k, qm) - lse)
            dss.append((p * (dot_nt(v, gm) - c)).astype(BF16))
            ps.append(p.astype(BF16))
            q_only.append(qm)
            g_only.append(gm)
        dv = dv + dot_nn(jnp.concatenate(ps, axis=1), jnp.concatenate(g_only, axis=0))
        dk = dk + dot_nn(jnp.concatenate(dss, axis=1), jnp.concatenate(q_only, axis=0))
    dk_ref[0] = dk.astype(BF16)
    dv_ref[0] = dv.astype(BF16)


def late(role, qd_o, stats, k, v, lo, dk_acc, dv_acc, dk_all, dv_all, head, first, after):
    n, seq, dim = dk_acc.shape
    pairs = dim // PAIR
    pick = lambda t: pl.BlockSpec((1, 1, seq, dim), lambda b, r: (t, b * (1 - r[0]), 0, 0))
    low_in = pl.BlockSpec((1, seq, dim), lambda b, r: (lo + b * (1 - r[0]), 0, 0))
    low = pl.BlockSpec((1, seq, dim), lambda b, r: (b * (1 - r[0]), 0, 0))
    still = pl.BlockSpec((1, seq, dim), lambda b, r: (first, 0, 0))
    out = pl.BlockSpec((1, seq, dim), lambda b, r: (first + b * (1 - r[0]), 0, 0))
    stat = pl.BlockSpec((1, pairs, 4, seq), lambda b, r: (b * (1 - r[0]), 0, 0, 0))
    return pl.pallas_call(
        functools.partial(late_kernel, head=head, scale=head ** -0.5),
        grid_spec=pltpu.PrefetchScalarGridSpec(
            num_scalar_prefetch=1,
            grid=(n,),
            in_specs=[pick(1), pick(0), stat, low_in, low_in, low, low, still, still] + [UNREAD] * len(after),
            out_specs=[out] * 2,
        ),
        out_shape=[jax.ShapeDtypeStruct(dk_all.shape, BF16)] * 2,
        input_output_aliases={8: 0, 9: 1},
        compiler_params=params(1),
        cost_estimate=pl.CostEstimate(flops=16 * n * seq * seq * dim, bytes_accessed=20 * n * seq * dim, transcendentals=0),
        name="late",
    )(role, qd_o, qd_o, stats, k, v, dk_acc, dv_acc, dk_all, dv_all, *after)


def split_rows(core_ref, full_ref, own_ref, send_ref):
    run = own_ref.shape[1]
    own_ref[0] = full_ref[pl.ds(pl.multiple_of(core_ref[0] * run, run), run), :]
    send_ref[0] = full_ref[pl.ds(pl.multiple_of((1 - core_ref[0]) * run, run), run), :]


def post_kernel(core_ref, a_ref, x_ref, wo_ref, bo_ref, *rest):
    own_ref, send_ref, full_ref = rest[-3:]
    out = dot_nn(a_ref[0], wo_ref[...]) + bo_ref[...]
    full_ref[...] = (x_ref[0].astype(F32) + out).astype(BF16)
    split_rows(core_ref, full_ref, own_ref, send_ref)


def row_outputs(n, run, dim):
    own = pl.BlockSpec((1, run, dim), lambda b, c: (c[0] * n + b, 0, 0))
    other = pl.BlockSpec((1, run, dim), lambda b, c: (b, 0, 0))
    return [own, other], [jax.ShapeDtypeStruct((2 * n, run, dim), BF16), jax.ShapeDtypeStruct((n, run, dim), BF16)]


def post(core, a, x, w_o, b_o, after):
    n, seq, dim = a.shape
    tok = pl.BlockSpec((1, seq, dim), lambda b, c: (b, 0, 0))
    whole = lambda shape: pl.BlockSpec(shape, lambda b, c: (0,) * len(shape))
    specs, shapes = row_outputs(n, seq // 2, dim)
    return pl.pallas_call(
        post_kernel,
        grid_spec=pltpu.PrefetchScalarGridSpec(
            num_scalar_prefetch=1,
            grid=(n,),
            in_specs=[tok, tok, whole((dim, dim)), whole((1, dim))] + [UNREAD] * len(after),
            out_specs=specs,
            scratch_shapes=[pltpu.VMEM((seq, dim), BF16)],
        ),
        out_shape=shapes,
        compiler_params=params(1),
        cost_estimate=pl.CostEstimate(flops=2 * n * seq * dim * dim, bytes_accessed=6 * n * seq * dim, transcendentals=0),
        name="post",
    )(core, a, x, w_o, b_o, *after)


def back_kernel(core_ref, dq_ref, dk_ref, dv_ref, x_ref, g_ref, lng_ref, w_ref, *rest):
    own_ref, send_ref, acc_ref, full_ref = rest[-4:]
    dim = x_ref.shape[2]

    @pl.when(pl.program_id(0) == 0)
    def _():
        acc_ref[...] = jnp.zeros_like(acc_ref)

    dh = dot_nn(dq_ref[0], w_ref[0:dim, :]) + dot_nn(dk_ref[0], w_ref[dim:2 * dim, :]) + dot_nn(dv_ref[0], w_ref[2 * dim:3 * dim, :])
    x_hat, inv_std = normed(x_ref[0].astype(F32))
    g = g_ref[0].astype(F32)
    u = dh * lng_ref[...]
    dx = inv_std * (u - jnp.mean(u, axis=-1, keepdims=True) - x_hat * jnp.mean(u * x_hat, axis=-1, keepdims=True))
    full_ref[...] = (g + dx).astype(BF16)
    split_rows(core_ref, full_ref, own_ref, send_ref)
    acc_ref[0:1, :] += jnp.sum(dh * x_hat, axis=0, keepdims=True)
    acc_ref[1:2, :] += jnp.sum(dh, axis=0, keepdims=True)
    for t, ref in enumerate((dq_ref, dk_ref, dv_ref)):
        acc_ref[2 + t:3 + t, :] += jnp.sum(ref[0].astype(F32), axis=0, keepdims=True)
    acc_ref[5:6, :] += jnp.sum(g, axis=0, keepdims=True)


def back(core, dq, dk, dv, x, g, ln_g, w_t, after):
    n, seq, dim = dq.shape
    tok = pl.BlockSpec((1, seq, dim), lambda b, c: (b, 0, 0))
    whole = lambda shape: pl.BlockSpec(shape, lambda b, c: (0,) * len(shape))
    specs, shapes = row_outputs(n, seq // 2, dim)
    return pl.pallas_call(
        back_kernel,
        grid_spec=pltpu.PrefetchScalarGridSpec(
            num_scalar_prefetch=1,
            grid=(n,),
            in_specs=[tok] * 5 + [whole((1, dim)), whole((3 * dim, dim))] + [UNREAD] * len(after),
            out_specs=specs + [whole((8, dim))],
            scratch_shapes=[pltpu.VMEM((seq, dim), BF16)],
        ),
        out_shape=shapes + [jax.ShapeDtypeStruct((8, dim), F32)],
        compiler_params=params(1),
        cost_estimate=pl.CostEstimate(flops=6 * n * seq * dim * dim, bytes_accessed=12 * n * seq * dim, transcendentals=0),
        name="back",
    )(core, dq, dk, dv, x, g, ln_g, w_t, *after)


def join_kernel(core_ref, *refs):
    own, other, (three_ref, one_ref) = refs[:4], refs[4:8], refs[8:]

    def put(parts):
        for t in range(3):
            three_ref[t, 0] = parts[t][...]
        one_ref[0] = parts[3][...]

    pl.when(pl.program_id(0) == 0)(lambda: put(own))
    pl.when(pl.program_id(0) == 1)(lambda: put(other))


def join(core, own, other):
    half, dim = own[0].shape
    rows = 128
    steps = half // rows
    mine = pl.BlockSpec((rows, dim), lambda j, r, c: (r * (1 - j) + (steps - 1) * j, 0))
    theirs = pl.BlockSpec((rows, dim), lambda j, r, c: (r * j, 0))
    side = lambda j, c: c[0] * (1 - j) + (1 - c[0]) * j
    three, one = pl.pallas_call(
        join_kernel,
        grid_spec=pltpu.PrefetchScalarGridSpec(
            num_scalar_prefetch=1,
            grid=(2, steps),
            in_specs=[mine] * 4 + [theirs] * 4,
            out_specs=[
                pl.BlockSpec((3, 1, rows, dim), lambda j, r, c: (0, side(j, c), r, 0)),
                pl.BlockSpec((1, rows, dim), lambda j, r, c: (side(j, c), r, 0)),
            ],
        ),
        out_shape=[jax.ShapeDtypeStruct((3, 2, half, dim), F32), jax.ShapeDtypeStruct((2, half, dim), F32)],
        compiler_params=params(2),
        cost_estimate=pl.CostEstimate(flops=8 * half * dim, bytes_accessed=64 * half * dim, transcendentals=0),
        name="join",
    )(core, *own, *other)
    return three.reshape(6 * half, dim), one.reshape(2 * half, dim)


def tok_dot(a, b):
    return lax.dot_general(a, b, (((0, 1), (0, 1)), ((), ())), preferred_element_type=F32)


def solution(mesh):
    tok_spec = P('dp', 'sp', None)
    part_spec = P('dp')

    def local_step(x, g, ln_g, ln_b, w_qkv, b_qkv, w_out, b_out):
        batch, _, dim = x.shape
        _, _, heads, head = w_qkv.shape
        index = lax.axis_index('sp')
        chip, core = lax.div(index, 2), lax.rem(index, 2)
        role, side = chip.reshape(1), core.reshape(1)
        ln_g2, ln_b2, b_o = ln_g.reshape(1, dim), ln_b.reshape(1, dim), b_out.reshape(1, dim)
        w_t = jnp.transpose(w_qkv, (1, 2, 3, 0)).reshape(3 * dim, dim)
        w_o = w_out.reshape(dim, dim)
        b_all = b_qkv.reshape(1, 3 * dim)
        half_b = batch // 2
        n = half_b // CHUNKS
        half_d = dim // 2

        def send(z, perm):
            return lax.ppermute(z, 'sp', perm)

        def handed(z, lo, count):
            return send(lax.dynamic_slice_in_dim(z, (1 - core) * half_b + lo, count, 0), SWAP_CORE)

        spans = ((0, n), (n, half_b - n))
        got = [(handed(g, *span), handed(x, *span)) for span in spans]
        fronts, whole = [], []
        for j, (lo, _) in enumerate(spans):
            *group, h, xb, gb = front(side, x, got[j][1], g, got[j][0], ln_g2, ln_b2, w_t, b_all, w_o, lo, whole)
            fronts.append(group)
            whole = [h, xb, gb]
        own, far = [], []
        for i in range(CHUNKS):
            (hs, qd, k, v), lo = fronts[min(i, 1)], max(i - 1, 0) * n
            own.append((qd, k, v, lo))
            far.append((send(hs[lo:lo + n], UP), send(qd[:, lo:lo + n], DOWN)))

        def halves_added(w):
            theirs = send(lax.dynamic_slice_in_dim(w, (1 - core) * half_d, half_d, 0), SWAP_CORE)
            return lax.dynamic_slice_in_dim(w, core * half_d, half_d, 0) + theirs

        accs, stats, sent = {}, {}, {}

        def forward(i, chain):
            k_o, v_o = other_kv(role, far[i][0], w_t, b_all)
            *chain, dk_acc, dv_acc, stats[i] = attend(role, *own[i], k_o, v_o, head, i * n, half_b, chain, [])
            accs[i] = dk_acc, dv_acc
            sent[i] = send(stats[i], DOWN)
            return chain

        def backward(i, chain, after):
            a, dq, dk, dv = chain
            _, k, v, lo = own[i]
            dk, dv = late(role, far[i][1], sent[i], k, v, lo, *accs[i], dk, dv, head, i * n, after)
            return [a, dq, dk, dv]

        chain = forward(0, [])
        chain = forward(1, chain)
        chain = forward(2, chain)
        chain = backward(0, chain, [])
        chain = forward(3, chain)

        dw_o = tok_dot(chain[0], gb)
        part_o = halves_added(dw_o)
        chain = backward(1, chain, [dw_o])
        chain = backward(2, chain, [])
        chain = backward(3, chain, [part_o])
        a, dq, dk, dv = chain
        sum_o = part_o + send(part_o, SWAP_CHIP)
        part_q = halves_added(tok_dot(dq, h))
        sum_q = part_q + send(part_q, SWAP_CHIP)
        part_k, part_v = halves_added(tok_dot(dk, h)), halves_added(tok_dot(dv, h))
        sum_k = part_k + send(part_k, SWAP_CHIP)
        sum_v = part_v + send(part_v, SWAP_CHIP)
        y = post(side, a, xb, w_o, b_o, [part_k, part_v])
        *d_x, acc = back(side, dq, dk, dv, xb, gb, ln_g2, w_t, [part_k, part_v])

        def joined(own_rows, other_rows):
            other_rows = send(other_rows, SWAP_CORE)
            return lax.dynamic_update_slice_in_dim(own_rows, other_rows, (1 - core) * half_b, 0)

        y, d_x = joined(*y), joined(*d_x)
        acc = acc + send(acc, SWAP_CORE)
        acc = acc + send(acc, SWAP_CHIP)

        sums = (sum_q, sum_k, sum_v, sum_o)
        dwt, d_w_out = join(side, sums, [send(w, SWAP_CORE) for w in sums])
        d_w_qkv = jnp.transpose(dwt.reshape(3, heads, head, dim), (3, 0, 1, 2))
        return y, d_x, acc[0], acc[1], d_w_qkv, acc[2:5].reshape(3, heads, head), d_w_out.reshape(heads, head, dim), acc[5]


    return jax.shard_map(local_step, mesh=mesh, in_specs=(tok_spec, tok_spec) + (P(),) * 6, out_specs=(tok_spec, tok_spec) + (part_spec,) * 6, check_vma=False)
```
